256 devices in a mesh: seq: 4 (over x_hi, core), ctx: 8 (over z), head: 8 (over x_lo, y).
Axes of the slice: x: 4 (x_hi: 2, x_lo: 2; x = x_hi * 2 + x_lo), y: 4, z: 8, core: 2. Of those that a mesh axis runs over, the one named last changes fastest.
Arguments:
- stream: bfloat16 [4, 512, 2880], P('seq', 'ctx'), may hold values from -6 to 6
- query_weight: bfloat16 [2880, 4096], P(None, 'head'), may hold values from -0.109375 to 0.109375
- cache_keys: bfloat16 [4, 16384, 8, 64], P('seq', 'ctx', 'head'), may hold values from -1000 to 1000
- cache_values: bfloat16 [4, 16384, 8, 64], P('seq', 'ctx', 'head'), may hold values from -6 to 6
- new_keys: bfloat16 [4, 512, 8, 64], P('seq', 'ctx', 'head'), may hold values from -18 to 18
- new_values: bfloat16 [4, 512, 8, 64], P('seq', 'ctx', 'head'), may hold values from -6 to 6
- out_weight: bfloat16 [4096, 2880], P('head'), may hold values from -0.09375 to 0.09375
- norm_gain: float32 [2880], replicated, may hold values from 0.5 to 1.5
- expert_ids: int32 [4, 512, 4], P('seq', 'ctx'), may hold values from 0 to 31, all different within a row; in each aligned block of 64 rows (0 to 63, 64 to 127, ..., all dimensions but the last counted through in order) at most 16 rows name the same one
- expert_weights: float32 [4, 512, 4], P('seq', 'ctx'), may hold values from 0.1 to 1
- gate_weight: bfloat16 [32, 2880, 2880], P(('seq', 'ctx'), None, 'head'), may hold values from -0.109375 to 0.109375
- up_weight: bfloat16 [32, 2880, 2880], P(('seq', 'ctx'), None, 'head'), may hold values from -0.109375 to 0.109375
- down_weight: bfloat16 [32, 2880, 2880], P(('seq', 'ctx'), 'head'), may hold values from -0.109375 to 0.109375
Outputs:
- mixed: bfloat16 [4, 512, 2880], P('seq', 'ctx', 'head')
The draws below stay inside these ranges and needn't reach their ends.
Inputs may be any that keep to these rules, and one draw needn't show every extreme that they name: `expert_ids`: in each aligned block of 64 rows (the tokens of one device) no expert is named by more than 16 rows; each row names 4 different experts.
All inputs are finite; a program needn't handle non-finite values.
Results may differ from the reference program's by a relative error of at most 0.015.
Values may be sent and summed in bfloat16 or wider, within the bound.
A program may use at most 64 MiB of HBM per device.

```python
import math
import jax
import jax.numpy as jnp
import numpy as np
from jax import lax

D = 2880
HEADS = 64
KV_HEADS = 8
HEAD_DIM = 64
FF = 2880
TOPK = 4
Q_DEV = 64
EXPERTS = 32
BATCH = 4
NEW = 512
CACHE = 16384
CAP = 16
N_CTX = 8
N_HEAD = 8


def draw_cache_keys(key, part):
    shape = (BATCH, CACHE, KV_HEADS, HEAD_DIM)
    base = 2.5 * jax.random.truncated_normal(jax.random.fold_in(key, 11), -6.0, 6.0, shape, jnp.float32)
    return jnp.clip(base, -1000.0, 1000.0).astype(jnp.bfloat16)


def block_scale(rng, dims, cuts, low, top_value):
    factor_of, own = 1.0, jax.random.fold_in(rng, 6)
    for dim, blocks in cuts:
        draws = jnp.exp(jax.random.uniform(jax.random.fold_in(own, dim), (blocks,), jnp.float32, low / len(cuts), top_value / len(cuts)))
        factor_of = factor_of * jnp.repeat(draws, dims[dim] // blocks).reshape([-1 if axis == dim else 1 for axis in range(len(dims))])
    return factor_of


def shared_out(own_key, own, number, rows, count, top, most, skew):
    order = jax.random.permutation(own_key, count)
    crowded, common = portions_of(count, rows * top, most, skew, True), portions_of(count, rows * top, most, skew, False)
    places = jnp.arange(count)

    def named(lengths, turn):
        used = int((lengths > 0).sum())
        fixed = max(1, used // 4)
        shifted = fixed + (places - fixed + turn * (used - fixed)) % max(1, count - fixed)
        return jnp.zeros((count,), jnp.int32).at[order[jnp.where(places < fixed, places, shifted)]].set(jnp.asarray(lengths, jnp.int32))

    lengths = jnp.where(number % 4 == 0, named(crowded, number // 4), named(common, number - number // 4 - 1))
    mixed = jax.random.permutation(jax.random.fold_in(own, 3), count)
    giver, receiver = mixed[0:count // 2 * 2:2], mixed[1:count // 2 * 2:2]
    room = jnp.minimum(lengths[giver] - 1, most - lengths[receiver]) // 2
    room = jnp.where((giver == order[0]) | (receiver == order[0]) | (lengths[receiver] == 0), 0, jnp.maximum(room, 0))
    shifted = jax.random.randint(jax.random.fold_in(own, 4), (count // 2,), 0, 1 << 20) % (room + 1)
    lengths = lengths.at[giver].add(-shifted).at[receiver].add(shifted)
    items = jnp.searchsorted(jnp.cumsum(lengths), jnp.arange(rows * top), side="right").astype(jnp.int32)
    grid = items.reshape(top, rows).T
    grid = grid[jax.random.permutation(jax.random.fold_in(own, 1), rows)]
    turn = jax.random.randint(jax.random.fold_in(own, 2), (rows, 1), 0, top)
    return jnp.take_along_axis(grid, (jnp.arange(top)[None, :] + turn) % top, axis=1)


def portions_of(amount, total, reach, skew, full):
    portions = [(1 << 20) // math.isqrt(grade ** skew) + 1 for grade in range(1, amount + 1)]
    largest = reach if full else min(reach, max(-(-total // amount), total * portions[0] // sum(portions)))
    least = 1 if total - largest >= amount - 1 else 0
    given, spare = [largest] + [least] * (amount - 1), total - largest - least * (amount - 1)
    while spare > 0:
        movable = [i for i in range(1, amount) if given[i] < largest] or [i for i in range(1, amount) if given[i] < reach]
        pool, left = sum([portions[i] for i in movable]), spare
        for i in movable:
            addition = min(reach - given[i], max(1, left * portions[i] // pool), spare)
            given[i] = given[i] + addition
            spare = spare - addition
    return np.array(given)


def bell_draw(own_key, dims, deviation, reach, shards=(), held_as=jnp.bfloat16):
    level = block_scale(own_key, dims, shards, -0.22, 0.18) if shards else 1.0
    values = jax.random.normal(own_key, dims, jnp.float32) * deviation * level
    return jnp.minimum(jnp.maximum(values, -reach), reach).astype(held_as)


def setup_inputs(seed: int = 0) -> dict:
    splits = jax.random.split(jax.random.key(seed), 14)
    stream = bell_draw(splits[0], (BATCH, NEW, D), 1.0, 6.0, ((0, 4), (1, 8)))
    query_weight = bell_draw(splits[1], (D, HEADS * HEAD_DIM), D ** -0.5, 0.109375, ((1, 8),))
    cache_keys = draw_cache_keys(jax.random.fold_in(splits[13], 71), 0)
    cache_values = bell_draw(splits[3], (BATCH, CACHE, KV_HEADS, HEAD_DIM), 1.0, 6.0, ((0, 4), (1, 8), (2, 8)))
    new_keys = bell_draw(splits[4], (BATCH, NEW, KV_HEADS, HEAD_DIM), 3.0, 18.0, ((0, 4), (1, 8), (2, 8)))
    new_values = bell_draw(splits[5], (BATCH, NEW, KV_HEADS, HEAD_DIM), 1.0, 6.0, ((0, 4), (1, 8), (2, 8)))
    out_weight = bell_draw(splits[6], (HEADS * HEAD_DIM, D), (HEADS * HEAD_DIM) ** -0.5, 0.09375, ((0, 8),))
    norm_gain = jnp.clip(1.0 + 0.1 * jax.random.normal(splits[7], (D,), jnp.float32), 0.5, 1.5)
    expert_ids_keys = jax.random.split(jax.random.fold_in(splits[8], 1), BATCH * NEW // Q_DEV)
    expert_ids_turns = jax.random.permutation(jax.random.fold_in(splits[8], 3), BATCH * NEW // Q_DEV)
    expert_ids = jax.vmap(lambda own, number: shared_out(jax.random.fold_in(splits[8], 2), own, number, Q_DEV, EXPERTS, TOPK, CAP, 2))(expert_ids_keys, expert_ids_turns).reshape((BATCH, NEW, TOPK))
    expert_weights = jnp.clip(jnp.exp(math.log(1.0) - 2.3025851 * jax.random.uniform(splits[9], (BATCH, NEW, TOPK), jnp.float32) ** block_scale(splits[9], (BATCH, NEW, TOPK), ((0, 4), (1, 8)), -0.2, 0.2)), 0.1, 1.0)
    gate_weight = bell_draw(splits[10], (EXPERTS, D, FF), D ** -0.5, 0.109375, ((0, 32), (2, 8)))
    up_weight = bell_draw(splits[11], (EXPERTS, D, FF), D ** -0.5, 0.109375, ((0, 32), (2, 8)))
    down_weight = bell_draw(splits[12], (EXPERTS, FF, D), FF ** -0.5, 0.109375, ((0, 32), (1, 8)))
    return dict(stream=stream, query_weight=query_weight, cache_keys=cache_keys, cache_values=cache_values, new_keys=new_keys, new_values=new_values, out_weight=out_weight, norm_gain=norm_gain, expert_ids=expert_ids, expert_weights=expert_weights, gate_weight=gate_weight, up_weight=up_weight, down_weight=down_weight)


def attend_sequence(operands):
    query, keys, values = operands
    group = HEADS // KV_HEADS
    span = CACHE + NEW
    key_pos = lax.broadcasted_iota(jnp.int32, (NEW, span), 1)
    tok_pos = lax.broadcasted_iota(jnp.int32, (NEW, span), 0)
    allowed = (key_pos < CACHE) | (key_pos - CACHE <= tok_pos)
    grouped = query.reshape(NEW, KV_HEADS, group, HEAD_DIM).transpose(1, 0, 2, 3)
    keyed = keys.transpose(1, 0, 2)
    valued = values.transpose(1, 0, 2)

    def per_head(pieces):
        block, head_keys, head_values = pieces
        scores = jnp.einsum('tgd,jd->tgj', block.astype(jnp.float32), head_keys.astype(jnp.float32)) * (1.0 / math.sqrt(HEAD_DIM))
        scores = jnp.where(allowed[:, None, :], scores, -jnp.inf)
        top = lax.optimization_barrier(jnp.max(scores, axis=-1))
        weights = jnp.exp(scores - top[..., None])
        total = lax.optimization_barrier(jnp.sum(weights, axis=-1))
        probs = weights.astype(jnp.bfloat16)
        numerator = jnp.einsum('tgj,jd->tgd', probs.astype(jnp.float32), head_values.astype(jnp.float32))
        return (numerator / total[..., None]).astype(jnp.bfloat16)
    heads_out = lax.map(per_head, (grouped, keyed, valued))
    return heads_out.transpose(1, 0, 2, 3).reshape(NEW, HEADS * HEAD_DIM)

def reference(stream, query_weight, cache_keys, cache_values, new_keys, new_values, out_weight, norm_gain, expert_ids, expert_weights, gate_weight, up_weight, down_weight):
    tokens = stream.reshape(BATCH * NEW, D)
    query = jnp.dot(tokens, query_weight, preferred_element_type=jnp.float32).astype(jnp.bfloat16)
    query = query.reshape(BATCH, NEW, HEADS * HEAD_DIM)
    keys = jnp.concatenate([cache_keys, new_keys], axis=1)
    values = jnp.concatenate([cache_values, new_values], axis=1)
    attn = lax.map(attend_sequence, (query, keys, values)).reshape(BATCH * NEW, HEADS * HEAD_DIM)
    resid = tokens.astype(jnp.float32) + jnp.dot(attn, out_weight, preferred_element_type=jnp.float32)
    normed = (resid * lax.rsqrt(lax.optimization_barrier(jnp.mean(resid * resid, axis=-1, keepdims=True)) + 1e-05) * norm_gain).astype(jnp.bfloat16)
    blocks = BATCH * N_CTX
    pairs = Q_DEV * TOPK
    chosen = expert_ids.reshape(blocks, pairs)
    onehot = (chosen[:, :, None] == lax.broadcasted_iota(jnp.int32, (1, 1, EXPERTS), 2)).astype(jnp.int32)
    before = jnp.cumsum(onehot, axis=1) - onehot
    slot = lax.optimization_barrier(jnp.sum(before * onehot, axis=-1)).astype(jnp.int32)
    block_of = lax.broadcasted_iota(jnp.int32, (blocks, pairs), 0)
    pair_of = lax.broadcasted_iota(jnp.int32, (blocks, pairs), 1)
    row = (block_of * CAP + slot).reshape(-1).astype(jnp.int32)
    token_of = (block_of * Q_DEV + pair_of // TOPK).reshape(-1).astype(jnp.int32)
    flat_chosen = chosen.reshape(-1).astype(jnp.int32)
    buffer = jnp.zeros((EXPERTS, blocks * CAP, D), jnp.bfloat16).at[flat_chosen, row].set(normed[token_of])
    share = FF // N_HEAD

    def expert(operands):
        rows, gate_w, up_w, down_w = operands
        gate = jnp.dot(rows, gate_w, preferred_element_type=jnp.float32)
        up = jnp.dot(rows, up_w, preferred_element_type=jnp.float32)
        hidden = (gate * jax.nn.sigmoid(1.702 * gate) * (up + 1.0)).astype(jnp.bfloat16)
        parts = jnp.einsum('rgf,gfd->grd', hidden.reshape(rows.shape[0], N_HEAD, share).astype(jnp.float32), down_w.reshape(N_HEAD, share, D).astype(jnp.float32))
        parts = lax.optimization_barrier(parts.astype(jnp.bfloat16))
        return lax.optimization_barrier(jnp.sum(parts.astype(jnp.float32), axis=0)).astype(jnp.bfloat16)
    expert_out = lax.map(expert, (buffer, gate_weight, up_weight, down_weight))
    picked = expert_out[flat_chosen, row].astype(jnp.float32).reshape(BATCH * NEW, TOPK, D)
    moe = lax.optimization_barrier(jnp.sum(expert_weights.reshape(BATCH * NEW, TOPK, 1) * picked, axis=1))
    return (resid + moe).astype(jnp.bfloat16).reshape(BATCH, NEW, D)
```

```python
import math

import jax
import jax.numpy as jnp
from jax import lax
from jax.experimental import pallas as pl
from jax.experimental.pallas import tpu as pltpu
from jax.sharding import PartitionSpec as P

CAP = 16
MESH = pl.DeviceIdType.MESH
LOG2E = 1.4426950408889634
NEG = -3.0e38
NT = (((1,), (1,)), ((), ()))


def remote(src, dst, send, recv, where):
    return pltpu.make_async_remote_copy(
        src_ref=src, dst_ref=dst, send_sem=send, recv_sem=recv, device_id=where, device_id_type=MESH
    )


def greet(groups):
    barrier = pltpu.get_barrier_semaphore()
    total = 0
    for axis in groups:
        size = lax.axis_size(axis)
        me = lax.axis_index(axis)
        for step in range(1, size):
            pl.semaphore_signal(
                barrier, inc=1, device_id={axis: lax.rem(me + step, size)}, device_id_type=MESH
            )
        total += size - 1
    return barrier, total


def attention_kernel(
    q_ref,
    kt_ref,
    vt_ref,
    nk_ref,
    nv_ref,
    own_ref,
    wo_hbm,
    resid_ref,
    qbuf,
    ke,
    ko,
    ve,
    vo,
    kn,
    vn,
    obuf,
    lbuf,
    rbuf,
    rlse,
    wo,
    pbuf,
    prec,
    q_send,
    q_recv,
    o_send,
    o_recv,
    l_send,
    l_recv,
    p_send,
    p_recv,
    wo_sem,
):
    n = lax.axis_size("ctx")
    place = lax.axis_index("ctx")
    heads = lax.axis_size("head")
    lane_of = lax.axis_index("head")
    barrier, total = greet(("ctx", "head"))
    wo_copy = pltpu.make_async_copy(wo_hbm, wo, wo_sem)
    wo_copy.start()
    rows = q_ref.shape[0]
    count = nk_ref.shape[0]
    half = kt_ref.shape[0]
    cached = kt_ref.shape[1]

    ke[0:half, :] = kt_ref[...]
    ke[half : 2 * half, :] = jnp.zeros((half, cached), jnp.bfloat16)
    ko[0:half, :] = jnp.zeros((half, cached), jnp.bfloat16)
    ko[half : 2 * half, :] = kt_ref[...]
    qbuf[0] = q_ref[...]
    low_n = lax.broadcasted_iota(jnp.int32, (count, 2 * half), 1) < half
    nk = nk_ref[...].astype(jnp.float32)
    nv = nv_ref[...].astype(jnp.float32)
    one = jnp.ones((count, 2 * half), jnp.float32)
    kn[0:count, :] = jnp.where(low_n, nk, 0.0).astype(jnp.bfloat16)
    kn[count : 2 * count, :] = jnp.where(low_n, 0.0, nk).astype(jnp.bfloat16)
    vn[0:count, 0 : 2 * half] = jnp.where(low_n, nv, 0.0).astype(jnp.bfloat16)
    vn[count : 2 * count, 0 : 2 * half] = jnp.where(low_n, 0.0, nv).astype(jnp.bfloat16)
    vn[0:count, 2 * half : 4 * half] = jnp.where(low_n, one, 0.0).astype(jnp.bfloat16)
    vn[count : 2 * count, 2 * half : 4 * half] = jnp.where(low_n, 0.0, one).astype(jnp.bfloat16)

    pl.semaphore_wait(barrier, total)
    right = lax.rem(place + 1, n)
    left = lax.rem(place + n - 1, n)
    remote(q_ref, qbuf.at[1], q_send.at[1], q_recv.at[1], {"ctx": right}).start()
    remote(q_ref, qbuf.at[2], q_send.at[2], q_recv.at[2], {"ctx": left}).start()

    wide = 256

    @pl.loop(0, cached // wide)
    def _(c):
        at = pl.ds(pl.multiple_of(c * wide, wide), wide)
        low = lax.broadcasted_iota(jnp.int32, (wide, 2 * half), 1) < half
        ones = jnp.where(low, 1.0, 0.0)
        v = vt_ref[:, at].astype(jnp.float32)
        blank = jnp.zeros_like(v)
        ve[at, 0 : 2 * half] = jnp.concatenate([v, blank], 0).T.astype(jnp.bfloat16)
        vo[at, 0 : 2 * half] = jnp.concatenate([blank, v], 0).T.astype(jnp.bfloat16)
        ve[at, 2 * half : 4 * half] = ones.astype(jnp.bfloat16)
        vo[at, 2 * half : 4 * half] = (1.0 - ones).astype(jnp.bfloat16)

    lane = lax.broadcasted_iota(jnp.int32, (rows, 2 * half), 1)
    low = lane < half
    tok = lax.rem(lax.broadcasted_iota(jnp.int32, (rows, 2 * half), 0), count)
    pos = lax.rem(lane, half)

    def offset_of(k):
        return lax.div(k + 1, 2) * (1 - 2 * lax.rem(k, 2))

    @pl.loop(0, n)
    def _(k):
        @pl.when(k > 0)
        def _():
            remote(
                qbuf.at[k], qbuf.at[k], q_send.at[k], q_recv.at[k], {"ctx": right}
            ).wait_recv()

            @pl.when(k + 2 < n)
            def _():
                onward = lax.rem(place + n + 1 - 2 * lax.rem(k + 1, 2), n)
                remote(
                    qbuf.at[k],
                    qbuf.at[k + 2],
                    q_send.at[k + 2],
                    q_recv.at[k + 2],
                    {"ctx": onward},
                ).start()

        source = lax.rem(place + offset_of(k) + n, n)
        q = qbuf[k]
        s_e = jnp.dot(q, ke[...], preferred_element_type=jnp.float32)
        s_o = jnp.dot(q, ko[...], preferred_element_type=jnp.float32)
        s_n = lax.dot_general(q, kn[...], NT, preferred_element_type=jnp.float32)
        ahead = jnp.where(place < source, count, jnp.where(place == source, 0, -count - 1))
        s_n = jnp.where(pos <= tok + ahead, s_n, NEG)
        m_e = jnp.maximum(
            jnp.max(s_e, axis=1, keepdims=True),
            jnp.max(jnp.where(low, s_n, NEG), axis=1, keepdims=True),
        )
        m_o = jnp.maximum(
            jnp.max(s_o, axis=1, keepdims=True),
            jnp.max(jnp.where(low, NEG, s_n), axis=1, keepdims=True),
        )
        p_e = jnp.exp2((s_e - m_e) * LOG2E).astype(jnp.bfloat16)
        p_o = jnp.exp2((s_o - m_o) * LOG2E).astype(jnp.bfloat16)
        tops = jnp.where(low, m_e, m_o)
        p_n = jnp.exp2((s_n - tops) * LOG2E).astype(jnp.bfloat16)
        acc = (
            jnp.dot(p_e, ve[...], preferred_element_type=jnp.float32)
            + jnp.dot(p_o, vo[...], preferred_element_type=jnp.float32)
            + jnp.dot(p_n, vn[...], preferred_element_type=jnp.float32)
        )
        num = acc[:, 0 : 2 * half]
        tot = acc[:, 2 * half : 4 * half]
        obuf[k] = (num / tot).astype(jnp.bfloat16)
        turned = (tops + jnp.log(tot)).T
        first = lax.broadcasted_iota(jnp.int32, (8, rows), 0) < 4
        lbuf[k] = jnp.where(first, turned[0:8, :], turned[half : half + 8, :])

        @pl.when(k > 0)
        def _():
            there = {"ctx": source}
            remote(obuf.at[k], rbuf.at[k], o_send.at[k], o_recv.at[k], there).start()
            remote(lbuf.at[k], rlse.at[k], l_send.at[k], l_recv.at[k], there).start()

    @pl.loop(1, n)
    def _(k):
        here = {"ctx": right}
        remote(obuf.at[k], rbuf.at[k], o_send.at[k], o_recv.at[k], here).wait_recv()
        remote(lbuf.at[k], rlse.at[k], l_send.at[k], l_recv.at[k], here).wait_recv()

    rbuf[0] = obuf[0]
    rlse[0] = lbuf[0]
    lse = [rlse[k] for k in range(n)]
    peak = lse[0]
    for k in range(1, n):
        peak = jnp.maximum(peak, lse[k])
    parts = [jnp.exp(x - peak) for x in lse]
    whole = parts[0]
    for k in range(1, n):
        whole = whole + parts[k]
    share = jnp.concatenate([x / whole for x in parts], axis=0)
    share = jnp.concatenate([share, share], axis=0).T
    upper = share.astype(jnp.bfloat16).astype(jnp.float32)
    first = lax.broadcasted_iota(jnp.int32, share.shape, 1) < 8 * n
    split = jnp.where(first, upper, share - upper).astype(jnp.bfloat16)
    col = lax.broadcasted_iota(jnp.int32, (16 * n, 2 * half * n), 1)
    row = lax.broadcasted_iota(jnp.int32, (16 * n, 2 * half * n), 0)
    wanted = lax.div(col, 2 * half) * 8 + jnp.where(lax.rem(col, 2 * half) < half, 0, 4)
    pick = jnp.where(lax.rem(row, 8 * n) == wanted, 1.0, 0.0).astype(jnp.bfloat16)
    factor = jnp.dot(split, pick, preferred_element_type=jnp.float32)
    attn = jnp.zeros((rows, 2 * half), jnp.float32)
    for k in range(n):
        attn = attn + factor[:, 2 * half * k : 2 * half * (k + 1)] * rbuf[k].astype(jnp.float32)
    attn = attn.astype(jnp.bfloat16)
    flat = jnp.concatenate([attn[count * j : count * (j + 1), :] for j in range(rows // count)], axis=1)

    wo_copy.wait()

    @pl.loop(0, heads - 1)
    def _(c):
        there = lax.rem(lane_of + 1 + c, heads)
        part = lax.dot_general(flat, wo[there], NT, preferred_element_type=jnp.float32)
        pbuf[c] = part.astype(jnp.bfloat16)
        remote(pbuf.at[c], prec.at[c], p_send.at[c], p_recv.at[c], {"head": there}).start()

    mine = lax.dot_general(flat, wo[lane_of], NT, preferred_element_type=jnp.float32)
    acc = own_ref[...] + mine
    for c in range(heads - 1):
        there = lax.rem(lane_of + 1 + c, heads)
        remote(pbuf.at[c], prec.at[c], p_send.at[c], p_recv.at[c], {"head": there}).wait_recv()
        acc = acc + prec[c].astype(jnp.float32)
    resid_ref[...] = acc

    @pl.loop(1, n)
    def _(k):
        here = {"ctx": right}
        remote(qbuf.at[k], qbuf.at[k], q_send.at[k], q_recv.at[k], here).wait_send()
        remote(obuf.at[k], rbuf.at[k], o_send.at[k], o_recv.at[k], here).wait_send()
        remote(lbuf.at[k], rlse.at[k], l_send.at[k], l_recv.at[k], here).wait_send()

    @pl.loop(0, heads - 1)
    def _(c):
        there = lax.rem(lane_of + 1 + c, heads)
        remote(pbuf.at[c], prec.at[c], p_send.at[c], p_recv.at[c], {"head": there}).wait_send()


def attend(q, kt, vt, nk, nv, own, wo):
    n = lax.axis_size("ctx")
    rows, wide = q.shape
    cached = kt.shape[1]
    count, width = own.shape
    heads = wo.shape[0]
    bf = jnp.bfloat16
    vm = pl.BlockSpec(memory_space=pltpu.VMEM)
    dma = pltpu.SemaphoreType.DMA
    return pl.pallas_call(
        attention_kernel,
        out_shape=jax.ShapeDtypeStruct((count, width), jnp.float32),
        in_specs=[vm] * 6 + [pl.BlockSpec(memory_space=pl.ANY)],
        out_specs=vm,
        scratch_shapes=[
            pltpu.VMEM((n, rows, wide), bf),
            pltpu.VMEM((wide, cached), bf),
            pltpu.VMEM((wide, cached), bf),
            pltpu.VMEM((cached, 2 * wide), bf),
            pltpu.VMEM((cached, 2 * wide), bf),
            pltpu.VMEM((2 * count, wide), bf),
            pltpu.VMEM((2 * count, 2 * wide), bf),
            pltpu.VMEM((n, rows, wide), bf),
            pltpu.VMEM((n, 8, rows), jnp.float32),
            pltpu.VMEM((n, rows, wide), bf),
            pltpu.VMEM((n, 8, rows), jnp.float32),
            pltpu.VMEM(wo.shape, bf),
            pltpu.VMEM((heads - 1, count, width), bf),
            pltpu.VMEM((heads - 1, count, width), bf),
            dma((n,)),
            dma((n,)),
            dma((n,)),
            dma((n,)),
            dma((n,)),
            dma((n,)),
            dma((heads - 1,)),
            dma((heads - 1,)),
            dma,
        ],
        compiler_params=pltpu.CompilerParams(
            collective_id=0, has_side_effects=True, vmem_limit_bytes=40 * 1024 * 1024
        ),
    )(q, kt, vt, nk, nv, own, wo)


def sent_to_all(array, axis):
    copies = jnp.broadcast_to(array, (lax.axis_size(axis), *array.shape))
    return lax.all_to_all(copies, axis, split_axis=0, concat_axis=0, tiled=True)


def joined_along(tiles, dim):
    shape = list(tiles.shape[1:])
    shape[dim] *= tiles.shape[0]
    return jnp.moveaxis(tiles, 0, dim).reshape(shape)


def gathered_copies(array, axis, dim):
    tiles = sent_to_all(array, axis)
    return joined_along(tiles, dim)


def split_up(array, dim, count):
    before, after = (array.shape[:dim], array.shape[dim + 1 :])
    return jnp.moveaxis(array.reshape(*before, count, -1, *after), dim, 0)


def sent_and_summed(array, axis, dim):
    tiles = split_up(array, dim, lax.axis_size(axis))
    arrived = lax.all_to_all(tiles, axis, split_axis=0, concat_axis=0, tiled=True)
    return arrived.astype(jnp.float32).sum(axis=0)


def taken_together(array, axis):
    return sent_to_all(array, axis).sum(axis=0)


def body(
    stream,
    query_weight,
    cache_keys,
    cache_values,
    new_keys,
    new_values,
    out_weight,
    norm_gain,
    expert_ids,
    expert_weights,
    gate_weight,
    up_weight,
    down_weight,
):
    tokens = stream[0]
    count = tokens.shape[0]
    model = tokens.shape[1]
    kv_local = cache_keys.shape[2]
    head_dim = cache_keys.shape[3]
    group = query_weight.shape[1] // (kv_local * head_dim)
    scale = 1.0 / math.sqrt(head_dim)
    heads = lax.axis_size("head")
    width = model // heads
    offset = lax.axis_index("head") * width
    query = jnp.dot(tokens, query_weight, preferred_element_type=jnp.float32).astype(jnp.bfloat16)
    query = query * jnp.bfloat16(scale)
    pairs = group * head_dim // 128
    query = query.reshape(count, pairs, 128).transpose(1, 0, 2).reshape(pairs * count, 128)
    fresh_keys = new_keys[0, :, 0, :]
    fresh_values = new_values[0, :, 0, :]
    own = lax.dynamic_slice_in_dim(tokens, offset, width, 1).astype(jnp.float32)
    resid_own = attend(
        query,
        cache_keys[0, :, 0, :].T,
        cache_values[0, :, 0, :].T,
        jnp.concatenate([fresh_keys, fresh_keys], axis=1),
        jnp.concatenate([fresh_values, fresh_values], axis=1),
        own,
        out_weight.T.reshape(heads, width, out_weight.shape[0]),
    )
    power = taken_together(jnp.sum(resid_own * resid_own, axis=-1), "head")
    gain_own = lax.dynamic_slice_in_dim(norm_gain, offset, width, 0)
    normed = (resid_own * lax.rsqrt(power[:, None] / model + 1e-05) * gain_own).astype(jnp.bfloat16)
    experts = lax.axis_size("seq") * lax.axis_size("ctx")
    slots = experts * CAP
    chosen = expert_ids[0].reshape(-1)
    onehot = (chosen[:, None] == lax.broadcasted_iota(jnp.int32, (1, experts), 1)).astype(jnp.int32)
    before = jnp.cumsum(onehot, axis=0) - onehot
    target = chosen * CAP + jnp.sum(before * onehot, axis=1)
    matches = target[None, :] == lax.broadcasted_iota(jnp.int32, (slots, 1), 0)
    select = jnp.sum(matches.astype(jnp.float32).reshape(slots, count, -1), axis=-1).astype(
        jnp.bfloat16
    )
    packed = jnp.dot(select, normed, preferred_element_type=jnp.float32).astype(jnp.bfloat16)
    packed = packed.reshape(experts, CAP, normed.shape[1])
    arrived = lax.all_to_all(packed, ("seq", "ctx"), split_axis=0, concat_axis=0, tiled=True)
    rows = arrived.reshape(slots, normed.shape[1])
    piece = lax.all_gather(rows, "head", axis=1, tiled=True)
    gate_rows = gate_weight[0]
    up_rows = up_weight[0]
    gate = jnp.dot(piece, gate_rows, preferred_element_type=jnp.float32)
    up = jnp.dot(piece, up_rows, preferred_element_type=jnp.float32)
    hidden = (gate * jax.nn.sigmoid(1.702 * gate) * (up + 1.0)).astype(jnp.bfloat16)
    columns = down_weight[0]
    expert_out = sent_and_summed(
        jnp.einsum("fd,rf->dr", columns, hidden, preferred_element_type=jnp.float32).astype(
            jnp.bfloat16
        ),
        "head",
        0,
    ).astype(jnp.bfloat16)
    returned = lax.all_to_all(expert_out, ("seq", "ctx"), split_axis=1, concat_axis=1, tiled=True)
    spread_weights = jnp.where(matches.T, expert_weights[0].reshape(-1)[:, None], 0.0)
    spread_weights = jnp.sum(spread_weights.reshape(count, -1, slots), axis=1)
    moe = lax.dot_general(
        spread_weights,
        returned.astype(jnp.float32),
        (((1,), (1,)), ((), ())),
        precision=lax.Precision.HIGHEST,
    )
    return (resid_own + moe).astype(jnp.bfloat16)[None]


def solution(mesh):
    in_specs = (
        P("seq", "ctx", None),
        P(None, "head"),
        P("seq", "ctx", "head", None),
        P("seq", "ctx", "head", None),
        P("seq", "ctx", "head", None),
        P("seq", "ctx", "head", None),
        P("head", None),
        P(),
        P("seq", "ctx", None),
        P("seq", "ctx", None),
        P(("seq", "ctx"), None, "head"),
        P(("seq", "ctx"), None, "head"),
        P(("seq", "ctx"), "head", None),
    )
    out_specs = P("seq", "ctx", "head")
    return jax.shard_map(body, mesh=mesh, in_specs=in_specs, out_specs=out_specs, check_vma=False)
```

```python
import math

import jax
import jax.numpy as jnp
from jax import lax
from jax.experimental import pallas as pl
from jax.experimental.pallas import tpu as pltpu
from jax.sharding import PartitionSpec as P

CAP = 16
MESH = pl.DeviceIdType.MESH
LOG2E = 1.4426950408889634
NEG = -3.0e38
NT = (((1,), (1,)), ((), ()))


def remote(src, dst, send, recv, where):
    return pltpu.make_async_remote_copy(
        src_ref=src, dst_ref=dst, send_sem=send, recv_sem=recv, device_id=where, device_id_type=MESH
    )


def greet(groups):
    barrier = pltpu.get_barrier_semaphore()
    total = 0
    for axis in groups:
        size = lax.axis_size(axis)
        me = lax.axis_index(axis)
        for step in range(1, size):
            pl.semaphore_signal(
                barrier, inc=1, device_id={axis: lax.rem(me + step, size)}, device_id_type=MESH
            )
        total += size - 1
    return barrier, total


def attention_kernel(
    q_ref,
    kt_ref,
    vt_ref,
    nk_ref,
    nv_ref,
    own_ref,
    wo_hbm,
    resid_ref,
    qbuf,
    ke,
    ko,
    ve,
    vo,
    kn,
    vn,
    obuf,
    lbuf,
    rbuf,
    rlse,
    wo,
    pbuf,
    prec,
    q_send,
    q_recv,
    o_send,
    o_recv,
    l_send,
    l_recv,
    p_send,
    p_recv,
    wo_sem,
):
    n = lax.axis_size("ctx")
    place = lax.axis_index("ctx")
    heads = lax.axis_size("head")
    lane_of = lax.axis_index("head")
    barrier, total = greet(("ctx", "head"))
    wo_copy = pltpu.make_async_copy(wo_hbm, wo, wo_sem)
    wo_copy.start()
    rows = q_ref.shape[0]
    count = nk_ref.shape[0]
    half = kt_ref.shape[0]
    cached = kt_ref.shape[1]

    ke[0:half, :] = kt_ref[...]
    ke[half : 2 * half, :] = jnp.zeros((half, cached), jnp.bfloat16)
    ko[0:half, :] = jnp.zeros((half, cached), jnp.bfloat16)
    ko[half : 2 * half, :] = kt_ref[...]
    qbuf[0] = q_ref[...]
    low_n = lax.broadcasted_iota(jnp.int32, (count, 2 * half), 1) < half
    nk = nk_ref[...].astype(jnp.float32)
    nv = nv_ref[...].astype(jnp.float32)
    one = jnp.ones((count, 2 * half), jnp.float32)
    kn[0:count, :] = jnp.where(low_n, nk, 0.0).astype(jnp.bfloat16)
    kn[count : 2 * count, :] = jnp.where(low_n, 0.0, nk).astype(jnp.bfloat16)
    vn[0:count, 0 : 2 * half] = jnp.where(low_n, nv, 0.0).astype(jnp.bfloat16)
    vn[count : 2 * count, 0 : 2 * half] = jnp.where(low_n, 0.0, nv).astype(jnp.bfloat16)
    vn[0:count, 2 * half : 4 * half] = jnp.where(low_n, one, 0.0).astype(jnp.bfloat16)
    vn[count : 2 * count, 2 * half : 4 * half] = jnp.where(low_n, 0.0, one).astype(jnp.bfloat16)

    pl.semaphore_wait(barrier, total)
    right = lax.rem(place + 1, n)
    left = lax.rem(place + n - 1, n)
    remote(q_ref, qbuf.at[1], q_send.at[1], q_recv.at[1], {"ctx": right}).start()
    remote(q_ref, qbuf.at[2], q_send.at[2], q_recv.at[2], {"ctx": left}).start()

    wide = 256

    @pl.loop(0, cached // wide)
    def _(c):
        at = pl.ds(pl.multiple_of(c * wide, wide), wide)
        low = lax.broadcasted_iota(jnp.int32, (wide, 2 * half), 1) < half
        ones = jnp.where(low, 1.0, 0.0)
        v = vt_ref[:, at].astype(jnp.float32)
        blank = jnp.zeros_like(v)
        ve[at, 0 : 2 * half] = jnp.concatenate([v, blank], 0).T.astype(jnp.bfloat16)
        vo[at, 0 : 2 * half] = jnp.concatenate([blank, v], 0).T.astype(jnp.bfloat16)
        ve[at, 2 * half : 4 * half] = ones.astype(jnp.bfloat16)
        vo[at, 2 * half : 4 * half] = (1.0 - ones).astype(jnp.bfloat16)

    lane = lax.broadcasted_iota(jnp.int32, (rows, 2 * half), 1)
    low = lane < half
    tok = lax.rem(lax.broadcasted_iota(jnp.int32, (rows, 2 * half), 0), count)
    pos = lax.rem(lane, half)

    def offset_of(k):
        return lax.div(k + 1, 2) * (1 - 2 * lax.rem(k, 2))

    @pl.loop(0, n)
    def _(k):
        @pl.when(k > 0)
        def _():
            remote(
                qbuf.at[k], qbuf.at[k], q_send.at[k], q_recv.at[k], {"ctx": right}
            ).wait_recv()

            @pl.when(k + 2 < n)
            def _():
                onward = lax.rem(place + n + 1 - 2 * lax.rem(k + 1, 2), n)
                remote(
                    qbuf.at[k],
                    qbuf.at[k + 2],
                    q_send.at[k + 2],
                    q_recv.at[k + 2],
                    {"ctx": onward},
                ).start()

        source = lax.rem(place + offset_of(k) + n, n)
        q = qbuf[k]
        s_e = jnp.dot(q, ke[...], preferred_element_type=jnp.float32)
        s_o = jnp.dot(q, ko[...], preferred_element_type=jnp.float32)
        s_n = lax.dot_general(q, kn[...], NT, preferred_element_type=jnp.float32)
        ahead = jnp.where(place < source, count, jnp.where(place == source, 0, -count - 1))
        s_n = jnp.where(pos <= tok + ahead, s_n, NEG)
        m_e = jnp.maximum(
            jnp.max(s_e, axis=1, keepdims=True),
            jnp.max(jnp.where(low, s_n, NEG), axis=1, keepdims=True),
        )
        m_o = jnp.maximum(
            jnp.max(s_o, axis=1, keepdims=True),
            jnp.max(jnp.where(low, NEG, s_n), axis=1, keepdims=True),
        )
        p_e = jnp.exp2((s_e - m_e) * LOG2E).astype(jnp.bfloat16)
        p_o = jnp.exp2((s_o - m_o) * LOG2E).astype(jnp.bfloat16)
        tops = jnp.where(low, m_e, m_o)
        p_n = jnp.exp2((s_n - tops) * LOG2E).astype(jnp.bfloat16)
        acc = (
            jnp.dot(p_e, ve[...], preferred_element_type=jnp.float32)
            + jnp.dot(p_o, vo[...], preferred_element_type=jnp.float32)
            + jnp.dot(p_n, vn[...], preferred_element_type=jnp.float32)
        )
        num = acc[:, 0 : 2 * half]
        tot = acc[:, 2 * half : 4 * half]
        obuf[k] = (num / tot).astype(jnp.bfloat16)
        turned = (tops + jnp.log(tot)).T
        first = lax.broadcasted_iota(jnp.int32, (8, rows), 0) < 4
        lbuf[k] = jnp.where(first, turned[0:8, :], turned[half : half + 8, :])

        @pl.when(k > 0)
        def _():
            there = {"ctx": source}
            remote(obuf.at[k], rbuf.at[k], o_send.at[k], o_recv.at[k], there).start()
            remote(lbuf.at[k], rlse.at[k], l_send.at[k], l_recv.at[k], there).start()

    @pl.loop(1, n)
    def _(k):
        here = {"ctx": right}
        remote(obuf.at[k], rbuf.at[k], o_send.at[k], o_recv.at[k], here).wait_recv()
        remote(lbuf.at[k], rlse.at[k], l_send.at[k], l_recv.at[k], here).wait_recv()

    rbuf[0] = obuf[0]
    rlse[0] = lbuf[0]
    lse = [rlse[k] for k in range(n)]
    peak = lse[0]
    for k in range(1, n):
        peak = jnp.maximum(peak, lse[k])
    parts = [jnp.exp(x - peak) for x in lse]
    whole = parts[0]
    for k in range(1, n):
        whole = whole + parts[k]
    share = jnp.concatenate([x / whole for x in parts], axis=0)
    share = jnp.concatenate([share, share], axis=0).T
    upper = share.astype(jnp.bfloat16).astype(jnp.float32)
    first = lax.broadcasted_iota(jnp.int32, share.shape, 1) < 8 * n
    split = jnp.where(first, upper, share - upper).astype(jnp.bfloat16)
    col = lax.broadcasted_iota(jnp.int32, (16 * n, 2 * half * n), 1)
    row = lax.broadcasted_iota(jnp.int32, (16 * n, 2 * half * n), 0)
    wanted = lax.div(col, 2 * half) * 8 + jnp.where(lax.rem(col, 2 * half) < half, 0, 4)
    pick = jnp.where(lax.rem(row, 8 * n) == wanted, 1.0, 0.0).astype(jnp.bfloat16)
    factor = jnp.dot(split, pick, preferred_element_type=jnp.float32)
    attn = jnp.zeros((rows, 2 * half), jnp.float32)
    for k in range(n):
        attn = attn + factor[:, 2 * half * k : 2 * half * (k + 1)] * rbuf[k].astype(jnp.float32)
    attn = attn.astype(jnp.bfloat16)
    flat = jnp.concatenate([attn[count * j : count * (j + 1), :] for j in range(rows // count)], axis=1)

    wo_copy.wait()

    @pl.loop(0, heads - 1)
    def _(c):
        there = lax.rem(lane_of + 1 + c, heads)
        part = lax.dot_general(flat, wo[there], NT, preferred_element_type=jnp.float32)
        pbuf[c] = part.astype(jnp.bfloat16)
        remote(pbuf.at[c], prec.at[c], p_send.at[c], p_recv.at[c], {"head": there}).start()

    mine = lax.dot_general(flat, wo[lane_of], NT, preferred_element_type=jnp.float32)
    acc = own_ref[...] + mine
    for c in range(heads - 1):
        there = lax.rem(lane_of + 1 + c, heads)
        remote(pbuf.at[c], prec.at[c], p_send.at[c], p_recv.at[c], {"head": there}).wait_recv()
        acc = acc + prec[c].astype(jnp.float32)
    resid_ref[...] = acc

    @pl.loop(1, n)
    def _(k):
        here = {"ctx": right}
        remote(qbuf.at[k], qbuf.at[k], q_send.at[k], q_recv.at[k], here).wait_send()
        remote(obuf.at[k], rbuf.at[k], o_send.at[k], o_recv.at[k], here).wait_send()
        remote(lbuf.at[k], rlse.at[k], l_send.at[k], l_recv.at[k], here).wait_send()

    @pl.loop(0, heads - 1)
    def _(c):
        there = lax.rem(lane_of + 1 + c, heads)
        remote(pbuf.at[c], prec.at[c], p_send.at[c], p_recv.at[c], {"head": there}).wait_send()


def attend(q, kt, vt, nk, nv, own, wo):
    n = lax.axis_size("ctx")
    rows, wide = q.shape
    cached = kt.shape[1]
    count, width = own.shape
    heads = wo.shape[0]
    bf = jnp.bfloat16
    vm = pl.BlockSpec(memory_space=pltpu.VMEM)
    dma = pltpu.SemaphoreType.DMA
    return pl.pallas_call(
        attention_kernel,
        out_shape=jax.ShapeDtypeStruct((count, width), jnp.float32),
        in_specs=[vm] * 6 + [pl.BlockSpec(memory_space=pl.ANY)],
        out_specs=vm,
        scratch_shapes=[
            pltpu.VMEM((n, rows, wide), bf),
            pltpu.VMEM((wide, cached), bf),
            pltpu.VMEM((wide, cached), bf),
            pltpu.VMEM((cached, 2 * wide), bf),
            pltpu.VMEM((cached, 2 * wide), bf),
            pltpu.VMEM((2 * count, wide), bf),
            pltpu.VMEM((2 * count, 2 * wide), bf),
            pltpu.VMEM((n, rows, wide), bf),
            pltpu.VMEM((n, 8, rows), jnp.float32),
            pltpu.VMEM((n, rows, wide), bf),
            pltpu.VMEM((n, 8, rows), jnp.float32),
            pltpu.VMEM(wo.shape, bf),
            pltpu.VMEM((heads - 1, count, width), bf),
            pltpu.VMEM((heads - 1, count, width), bf),
            dma((n,)),
            dma((n,)),
            dma((n,)),
            dma((n,)),
            dma((n,)),
            dma((n,)),
            dma((heads - 1,)),
            dma((heads - 1,)),
            dma,
        ],
        compiler_params=pltpu.CompilerParams(
            collective_id=0, has_side_effects=True, vmem_limit_bytes=40 * 1024 * 1024
        ),
    )(q, kt, vt, nk, nv, own, wo)


GROUPS = 4


def expert_kernel(
    resid_ref,
    gain_ref,
    ids_ref,
    weights_ref,
    gate_hbm,
    up_hbm,
    down_hbm,
    out_ref,
    raw,
    wide,
    wgu,
    wdn,
    packed,
    xall,
    acc,
    hidden,
    sbuf,
    rbuf,
    final,
    back,
    w_sem,
    d_send,
    d_recv,
    g_send,
    g_recv,
    s_send,
    s_recv,
    b_send,
    b_recv,
):
    seqs, ctxs, heads = lax.axis_size("seq"), lax.axis_size("ctx"), lax.axis_size("head")
    s, c, h = lax.axis_index("seq"), lax.axis_index("ctx"), lax.axis_index("head")
    experts = seqs * ctxs
    count, width = resid_ref.shape
    padded = wide.shape[1]
    block = ctxs * CAP
    f32, bf = jnp.float32, jnp.bfloat16
    ring = heads // 2
    col, y = lax.div(h, ring), lax.rem(h, ring)

    def head_at(across, dy):
        return (col if across == 0 else 1 - col) * ring + lax.rem(y + dy + ring, ring)

    other, above, below = head_at(1, 0), head_at(0, 1), head_at(0, -1)
    barrier = pltpu.get_barrier_semaphore()

    @pl.loop(1, experts)
    def _(step):
        there = {
            "seq": lax.rem(s + lax.div(step, ctxs), seqs),
            "ctx": lax.rem(c + lax.rem(step, ctxs), ctxs),
        }
        pl.semaphore_signal(barrier, inc=1, device_id=there, device_id_type=MESH)

    for peer in (other, above, below):
        pl.semaphore_signal(barrier, inc=1, device_id={"head": peer}, device_id_type=MESH)
    loads = [
        pltpu.make_async_copy(source, raw.at[i], w_sem.at[i])
        for i, source in enumerate((gate_hbm, up_hbm, down_hbm))
    ]
    for load in loads:
        load.start()

    ids = ids_ref[...]
    given = weights_ref[...]
    index = lax.broadcasted_iota(jnp.int32, (count, experts), 1)
    named = jnp.zeros((count, experts), f32)
    amount = jnp.zeros((count, experts), f32)
    for j in range(ids.shape[1]):
        hit = ids[:, j : j + 1] == index
        named = named + jnp.where(hit, 1.0, 0.0)
        amount = amount + jnp.where(hit, given[:, j : j + 1], 0.0)
    before = jnp.where(
        lax.broadcasted_iota(jnp.int32, (count, count), 1)
        < lax.broadcasted_iota(jnp.int32, (count, count), 0),
        1.0,
        0.0,
    ).astype(bf)
    rank = jnp.dot(before, named.astype(bf), preferred_element_type=f32)
    key = jnp.where(named > 0.5, rank, 128.0)
    spread = jnp.where(
        lax.div(lax.broadcasted_iota(jnp.int32, (experts, experts * CAP), 1), CAP)
        == lax.broadcasted_iota(jnp.int32, (experts, experts * CAP), 0),
        1.0,
        0.0,
    ).astype(bf)
    key = jnp.dot(key.astype(bf), spread, preferred_element_type=f32)
    slot = lax.rem(lax.broadcasted_iota(jnp.int32, (count, experts * CAP), 1), CAP).astype(f32)
    chosen = key == slot
    select = jnp.where(chosen, 1.0, 0.0).T.astype(bf)

    def pieces(x):
        one = x.astype(bf)
        rest = x - one.astype(f32)
        two = rest.astype(bf)
        return one, two, (rest - two.astype(f32)).astype(bf)

    factors = []
    for piece in pieces(amount):
        on_slots = jnp.dot(piece, spread, preferred_element_type=f32)
        factors.append(jnp.where(chosen, on_slots, 0.0).astype(bf))

    resid = resid_ref[...]
    wide[...] = jnp.zeros(wide.shape, f32)
    wide[:, 0:width] = resid * gain_ref[...]
    power = jnp.sum(resid * resid, axis=1, keepdims=True)
    lane = lax.broadcasted_iota(jnp.int32, (count, padded), 1)
    row = wide[...]
    for i, piece in enumerate(pieces(power)):
        row = jnp.where(lane == width + i, piece.astype(f32), row)
    packed[...] = jnp.dot(select, row.astype(bf), preferred_element_type=f32).astype(bf)

    me = s * ctxs + c
    mine = pl.ds(pl.multiple_of(me * CAP, CAP), CAP)
    pl.semaphore_wait(barrier, experts - 1 + 3)

    @pl.loop(1, experts)
    def _(step):
        s_to = lax.rem(s + seqs - lax.div(step, ctxs), seqs)
        c_to = lax.rem(c + lax.rem(step, ctxs), ctxs)
        at = pl.ds(pl.multiple_of((s_to * ctxs + c_to) * CAP, CAP), CAP)
        remote(
            packed.at[at], xall.at[0, mine], d_send.at[step], d_recv.at[step], {"seq": s_to, "ctx": c_to}
        ).start()

    xall[0, mine] = packed[mine]

    for load in loads:
        load.wait()
    tail = jnp.zeros((width, padded - width), bf)
    foot = jnp.zeros((padded - width, padded), bf)
    for i in range(heads):
        for j in range(2):
            wgu[i, j * padded : j * padded + width, :] = jnp.concatenate(
                [raw[j, :, i * width : (i + 1) * width], tail], axis=1
            )
            wgu[i, j * padded + width : (j + 1) * padded, :] = foot

    def rows_of(g):
        return pl.ds(pl.multiple_of(lax.rem(s + g, seqs) * block, block), block)

    def gather(kind, g, source, target):
        at = rows_of(g)
        return remote(
            xall.at[source, at],
            xall.at[kind, at],
            g_send.at[kind, g],
            g_recv.at[kind, g],
            {"head": target},
        )

    def stage_a(g):
        @pl.loop(1 if g == 0 else 0, ctxs)
        def _(dc):
            step = g * ctxs + dc
            at = pl.ds(0, CAP)
            remote(
                packed.at[at], xall.at[0, mine], d_send.at[step], d_recv.at[step], {"ctx": lax.rem(c + 1, ctxs)}
            ).wait_recv()

        gather(1, g, 0, other).start()
        gather(2, g, 0, above).start()
        gather(3, g, 0, below).start()

    def stage_b(g):
        gather(1, g, 0, other).wait_recv()
        gather(4, g, 1, above).start()
        gather(5, g, 1, below).start()
        gather(2, g, 0, above).wait_recv()
        gather(3, g, 0, below).wait_recv()
        if g % 2 == 0:
            gather(6, g, 2, above).start()
        else:
            gather(6, g, 3, below).start()

    def stage_c(g):
        gather(6, g, 2, above).wait_recv()
        gather(7, g, 6, other).start()

    place = [h, other, below, above, head_at(1, -1), head_at(1, 1), head_at(0, 2), head_at(1, 2)]

    def absorb(low, high):
        @pl.loop(low, high)
        def _(kind):
            where = place[low]
            for k in range(low + 1, high):
                where = jnp.where(kind == k, place[k], where)
            update = lax.dot_general(xall[kind], wgu[where], NT, preferred_element_type=f32)
            if low == 0:
                acc[...] = update
            else:
                acc[...] += update

    stage_a(0)
    stage_a(1)
    stage_b(0)
    stage_a(2)
    stage_b(1)
    stage_c(0)
    stage_a(3)
    for i in range(heads):
        wdn[i, 0:width, :] = jnp.concatenate([raw[2, :, i * width : (i + 1) * width], tail], axis=1)
        wdn[i, width:padded, :] = foot
    stage_b(2)
    stage_c(1)
    absorb(0, 1)
    stage_b(3)
    stage_c(2)
    absorb(1, 4)
    stage_c(3)
    for g in range(GROUPS):
        gather(4, g, 1, above).wait_recv()
        gather(5, g, 1, below).wait_recv()
    absorb(4, 7)
    for g in range(GROUPS):
        gather(7, g, 6, other).wait_recv()
    absorb(7, 8)

    @pl.loop(0, GROUPS)
    def _(g):
        at = pl.ds(pl.multiple_of(g * block, block), block)
        tile = jnp.zeros((block, 128), f32)
        for k in range(heads):
            tile = tile + xall[k, at, padded - 128 : padded].astype(f32)
        spot = lax.broadcasted_iota(jnp.int32, (block, 128), 1) + (padded - 128)
        tile = jnp.where((spot >= width) & (spot < width + 3), tile, 0.0)
        power = jnp.sum(tile, axis=1, keepdims=True)
        scale = lax.rsqrt(power / (width * heads) + 1e-05)
        gate = acc[at, 0:padded] * scale
        up = acc[at, padded : 2 * padded] * scale
        hidden[at] = (gate * jax.nn.sigmoid(1.702 * gate) * (up + 1.0)).astype(bf)

    def part(g, target):
        return jnp.dot(hidden[rows_of(g)], wdn[target], preferred_element_type=f32)

    def scatter(kind, g, target):
        return remote(
            sbuf.at[kind, g], rbuf.at[kind, g], s_send.at[kind, g], s_recv.at[kind, g], {"head": target}
        )

    def got(kind, g):
        scatter(kind, g, other).wait_recv()
        return rbuf[kind, g].astype(f32)

    def send(kind, g, value, target):
        sbuf[kind, g] = value.astype(bf)
        scatter(kind, g, target).start()

    @pl.loop(0, GROUPS + 3)
    def _(t):
        @pl.when(t < GROUPS)
        def _():
            g = t
            even = lax.rem(g, 2) == 0
            send(0, g, part(g, head_at(1, 2)), other)
            send(1, g, part(g, head_at(1, -1)), below)
            send(2, g, part(g, head_at(1, 1)), above)

            @pl.when(even)
            def _():
                send(5, g, part(g, below), below)

            @pl.when(jnp.logical_not(even))
            def _():
                send(6, g, part(g, above), above)

        @pl.when((t >= 1) & (t < GROUPS + 1))
        def _():
            g = t - 1
            even = lax.rem(g, 2) == 0
            value = part(g, head_at(0, 2)) + got(0, g)
            send(3, g, value, jnp.where(even, above, below))
            value = part(g, other) + got(1, g) + got(2, g)
            send(4, g, value, other)

        @pl.when((t >= 2) & (t < GROUPS + 2))
        def _():
            g = t - 2
            even = lax.rem(g, 2) == 0

            @pl.when(even)
            def _():
                send(6, g, part(g, above) + got(3, g), above)

            @pl.when(jnp.logical_not(even))
            def _():
                send(5, g, part(g, below) + got(3, g), below)

        @pl.when(t >= 3)
        def _():
            g = t - 3
            value = part(g, h) + got(4, g) + got(5, g) + got(6, g)
            final[rows_of(g)] = value.astype(bf)
            s_to = lax.rem(s + g, seqs)

            @pl.loop(0, ctxs)
            def _(dc):
                @pl.when(g * ctxs + dc > 0)
                def _():
                    step = g * ctxs + dc
                    c_to = lax.rem(c + dc, ctxs)
                    at = pl.ds(pl.multiple_of((s_to * ctxs + c_to) * CAP, CAP), CAP)
                    remote(
                        final.at[at], back.at[mine], b_send.at[step], b_recv.at[step], {"seq": s_to, "ctx": c_to}
                    ).start()

    back[mine] = final[mine]

    def returned(step):
        at = pl.ds(0, CAP)
        return remote(
            final.at[at], back.at[mine], b_send.at[step], b_recv.at[step], {"ctx": lax.rem(c + 1, ctxs)}
        )

    @pl.loop(1, experts)
    def _(step):
        returned(step).wait_recv()

    moe = jnp.zeros((count, padded), f32)
    for factor in factors:
        moe = moe + jnp.dot(factor, back[...], preferred_element_type=f32)
    out_ref[...] = (resid + moe[:, 0:width]).astype(bf)

    @pl.loop(1, experts)
    def _(step):
        at = pl.ds(0, CAP)
        remote(
            packed.at[at], xall.at[0, mine], d_send.at[step], d_recv.at[step], {"ctx": lax.rem(c + 1, ctxs)}
        ).wait_send()
        returned(step).wait_send()

    for g in range(GROUPS):
        for kind in range(1, heads):
            gather(kind, g, 0, other).wait_send()
        for kind in range(heads - 1):
            scatter(kind, g, other).wait_send()


def route(resid, gain, ids, weights, gate, up, down):
    seqs, ctxs, heads = lax.axis_size("seq"), lax.axis_size("ctx"), lax.axis_size("head")
    experts = seqs * ctxs
    slots = experts * CAP
    count, width = resid.shape
    hidden, model = gate.shape
    padded = -(-(width + 3) // 128) * 128
    block = ctxs * CAP
    bf, f32 = jnp.bfloat16, jnp.float32
    vm = pl.BlockSpec(memory_space=pltpu.VMEM)
    dma = pltpu.SemaphoreType.DMA
    return pl.pallas_call(
        expert_kernel,
        out_shape=jax.ShapeDtypeStruct((count, width), bf),
        in_specs=[vm] * 4 + [pl.BlockSpec(memory_space=pl.ANY)] * 3,
        out_specs=vm,
        scratch_shapes=[
            pltpu.VMEM((3, hidden, model), bf),
            pltpu.VMEM((count, padded), f32),
            pltpu.VMEM((heads, 2 * padded, padded), bf),
            pltpu.VMEM((heads, padded, padded), bf),
            pltpu.VMEM((slots, padded), bf),
            pltpu.VMEM((heads, slots, padded), bf),
            pltpu.VMEM((slots, 2 * padded), f32),
            pltpu.VMEM((slots, padded), bf),
            pltpu.VMEM((heads - 1, GROUPS, block, padded), bf),
            pltpu.VMEM((heads - 1, GROUPS, block, padded), bf),
            pltpu.VMEM((slots, padded), bf),
            pltpu.VMEM((slots, padded), bf),
            dma((3,)),
            dma((experts,)),
            dma((experts,)),
            dma((heads, GROUPS)),
            dma((heads, GROUPS)),
            dma((heads - 1, GROUPS)),
            dma((heads - 1, GROUPS)),
            dma((experts,)),
            dma((experts,)),
        ],
        compiler_params=pltpu.CompilerParams(
            collective_id=1, has_side_effects=True, vmem_limit_bytes=48 * 1024 * 1024
        ),
    )(resid, gain, ids, weights, gate, up, down)


def body(
    stream,
    query_weight,
    cache_keys,
    cache_values,
    new_keys,
    new_values,
    out_weight,
    norm_gain,
    expert_ids,
    expert_weights,
    gate_weight,
    up_weight,
    down_weight,
):
    tokens = stream[0]
    count, model = tokens.shape
    kv_local, head_dim = cache_keys.shape[2:]
    group = query_weight.shape[1] // (kv_local * head_dim)
    heads = lax.axis_size("head")
    width = model // heads
    offset = lax.axis_index("head") * width
    scale = 1.0 / math.sqrt(head_dim)
    query = jnp.dot(tokens, query_weight, preferred_element_type=jnp.float32).astype(jnp.bfloat16)
    query = query * jnp.bfloat16(scale)
    pairs = group * head_dim // 128
    query = query.reshape(count, pairs, 128).transpose(1, 0, 2).reshape(pairs * count, 128)
    fresh_keys = new_keys[0, :, 0, :]
    fresh_values = new_values[0, :, 0, :]
    own = lax.dynamic_slice_in_dim(tokens, offset, width, 1).astype(jnp.float32)
    gain = lax.dynamic_slice_in_dim(norm_gain, offset, width, 0)[None]
    resid = attend(
        query,
        cache_keys[0, :, 0, :].T,
        cache_values[0, :, 0, :].T,
        jnp.concatenate([fresh_keys, fresh_keys], axis=1),
        jnp.concatenate([fresh_values, fresh_values], axis=1),
        own,
        out_weight.T.reshape(heads, width, out_weight.shape[0]),
    )
    mixed = route(
        resid,
        gain,
        expert_ids[0],
        expert_weights[0],
        gate_weight[0].T,
        up_weight[0].T,
        down_weight[0],
    )
    return mixed[None]


def solution(mesh):
    in_specs = (
        P("seq", "ctx", None),
        P(None, "head"),
        P("seq", "ctx", "head", None),
        P("seq", "ctx", "head", None),
        P("seq", "ctx", "head", None),
        P("seq", "ctx", "head", None),
        P("head", None),
        P(),
        P("seq", "ctx", None),
        P("seq", "ctx", None),
        P(("seq", "ctx"), None, "head"),
        P(("seq", "ctx"), None, "head"),
        P(("seq", "ctx"), "head", None),
    )
    out_specs = P("seq", "ctx", "head")
    return jax.shard_map(body, mesh=mesh, in_specs=in_specs, out_specs=out_specs, check_vma=False)
```

```python
import math

import jax
import jax.numpy as jnp
from jax import lax
from jax.experimental import pallas as pl
from jax.experimental.pallas import tpu as pltpu
from jax.sharding import PartitionSpec as P

CAP = 16
MESH = pl.DeviceIdType.MESH
LOG2E = 1.4426950408889634
NEG = -3.0e38
NT = (((1,), (1,)), ((), ()))
GROUPS = 4
DEPTH = 768


def remote(src, dst, send, recv, where):
    return pltpu.make_async_remote_copy(
        src_ref=src, dst_ref=dst, send_sem=send, recv_sem=recv, device_id=where, device_id_type=MESH
    )


def layer_kernel(
    tok_hbm,
    qw_hbm,
    kt_hbm,
    vt_hbm,
    nk_ref,
    nv_ref,
    wo_hbm,
    gain_ref,
    ids_ref,
    weights_ref,
    gate_hbm,
    up_hbm,
    down_hbm,
    out_ref,
    tok,
    qw,
    vt,
    own,
    gain,
    resid_s,
    qbuf,
    ke,
    ko,
    ve,
    vo,
    kn,
    vn,
    s_low,
    s_high,
    s_new,
    tops,
    level,
    p_new,
    half_acc,
    obuf,
    lbuf,
    rbuf_o,
    rlse,
    wo,
    pbuf,
    prec,
    raw,
    wide,
    wgu,
    wdn,
    select_s,
    factor_s,
    packed,
    xall,
    acc,
    hidden,
    sbuf,
    rbuf,
    final,
    back,
    in_sem,
    q_send,
    q_recv,
    o_send,
    o_recv,
    l_send,
    l_recv,
    p_send,
    p_recv,
    w_sem,
    d_send,
    d_recv,
    g_send,
    g_recv,
    s_send,
    s_recv,
    b_send,
    b_recv,
):
    seqs, ctxs, heads = lax.axis_size("seq"), lax.axis_size("ctx"), lax.axis_size("head")
    s, c, h = lax.axis_index("seq"), lax.axis_index("ctx"), lax.axis_index("head")
    n, place, lane_of = ctxs, c, h
    experts = seqs * ctxs
    count, model = tok.shape
    width = own.shape[1]
    padded = wide.shape[1]
    block = ctxs * CAP
    f32, bf = jnp.float32, jnp.bfloat16
    ring = heads // 2
    col, y = lax.div(h, ring), lax.rem(h, ring)
    rows = qbuf.shape[1]
    half = ke.shape[0] // 2
    cached = ke.shape[1]
    pair = 2 * half

    def head_at(across, dy):
        return (col if across == 0 else 1 - col) * ring + lax.rem(y + dy + ring, ring)

    other, above, below = head_at(1, 0), head_at(0, 1), head_at(0, -1)
    edges = list(range(0, model, DEPTH)) + [model]
    spans = list(zip(edges[:-1], edges[1:]))
    tok_load = pltpu.make_async_copy(tok_hbm, tok, in_sem.at[0])
    qw_loads = [
        pltpu.make_async_copy(qw_hbm.at[low:high], qw.at[low:high], in_sem.at[4 + i])
        for i, (low, high) in enumerate(spans)
    ]
    kv_loads = [
        pltpu.make_async_copy(kt_hbm, ke.at[0:half], in_sem.at[1]),
        pltpu.make_async_copy(kt_hbm, ko.at[half:pair], in_sem.at[2]),
        pltpu.make_async_copy(vt_hbm, vt, in_sem.at[3]),
    ]
    for load in [tok_load] + qw_loads + kv_loads:
        load.start()
    wo_copy = pltpu.make_async_copy(wo_hbm, wo, w_sem.at[3])
    loads = [
        pltpu.make_async_copy(source, raw.at[i], w_sem.at[i])
        for i, source in enumerate((gate_hbm, up_hbm, down_hbm))
    ]
    barrier = pltpu.get_barrier_semaphore()

    @pl.loop(1, experts)
    def _(step):
        there = {
            "seq": lax.rem(s + lax.div(step, ctxs), seqs),
            "ctx": lax.rem(c + lax.rem(step, ctxs), ctxs),
        }
        pl.semaphore_signal(barrier, inc=1, device_id=there, device_id_type=MESH)

    @pl.loop(1, heads)
    def _(step):
        there = {"head": lax.rem(h + step, heads)}
        pl.semaphore_signal(barrier, inc=1, device_id=there, device_id_type=MESH)

    ke[half:pair, :] = jnp.zeros((half, cached), bf)
    ko[0:half, :] = jnp.zeros((half, cached), bf)
    low_n = lax.broadcasted_iota(jnp.int32, (count, pair), 1) < half
    nk = nk_ref[...].astype(f32)
    nk = jnp.concatenate([nk, nk], axis=1)
    nv = nv_ref[...].astype(f32)
    nv = jnp.concatenate([nv, nv], axis=1)
    kn[0:count, :] = jnp.where(low_n, nk, 0.0).astype(bf)
    kn[count : 2 * count, :] = jnp.where(low_n, 0.0, nk).astype(bf)
    vn[0:count, 0:pair] = jnp.where(low_n, nv, 0.0).astype(bf)
    vn[count : 2 * count, 0:pair] = jnp.where(low_n, 0.0, nv).astype(bf)
    vn[0:count, pair : 2 * pair] = jnp.where(low_n, 1.0, 0.0).astype(bf)
    vn[count : 2 * count, pair : 2 * pair] = jnp.where(low_n, 0.0, 1.0).astype(bf)

    tok_load.wait()
    query = jnp.zeros((count, qw.shape[1]), f32)
    for (low_k, high_k), load in zip(spans, qw_loads):
        load.wait()
        query = query + jnp.dot(tok[:, low_k:high_k], qw[low_k:high_k, :], preferred_element_type=f32)
    query = (query.astype(bf).astype(f32) * (1.0 / math.sqrt(half))).astype(bf)
    for j in range(rows // count):
        qbuf[0, count * j : count * (j + 1), :] = query[:, pair * j : pair * (j + 1)]
    for load in kv_loads:
        load.wait()

    pl.semaphore_wait(barrier, experts - 1 + heads - 1)
    right = lax.rem(place + 1, n)
    left = lax.rem(place + n - 1, n)
    remote(qbuf.at[0], qbuf.at[1], q_send.at[1], q_recv.at[1], {"ctx": right}).start()
    remote(qbuf.at[0], qbuf.at[2], q_send.at[2], q_recv.at[2], {"ctx": left}).start()
    wo_copy.start()
    for load in loads:
        load.start()

    span = 256

    @pl.loop(0, cached // span)
    def _(i):
        at = pl.ds(pl.multiple_of(i * span, span), span)
        ones = jnp.where(lax.broadcasted_iota(jnp.int32, (span, pair), 1) < half, 1.0, 0.0)
        v = vt[:, at].astype(f32)
        blank = jnp.zeros_like(v)
        ve[at, 0:pair] = jnp.concatenate([v, blank], 0).T.astype(bf)
        vo[at, 0:pair] = jnp.concatenate([blank, v], 0).T.astype(bf)
        ve[at, pair : 2 * pair] = ones.astype(bf)
        vo[at, pair : 2 * pair] = (1.0 - ones).astype(bf)

    lane = lax.broadcasted_iota(jnp.int32, (rows, pair), 1)
    low = lane < half
    tokpos = lax.rem(lax.broadcasted_iota(jnp.int32, (rows, pair), 0), count)
    pos = lax.rem(lane, half)

    def source_of(k):
        return lax.rem(place + lax.div(k + 1, 2) * (1 - 2 * lax.rem(k, 2)) + n, n)

    def score_even(k, turn):
        q = qbuf[k]
        source = source_of(k)
        fresh = lax.dot_general(q, kn[...], NT, preferred_element_type=f32)
        ahead = jnp.where(place < source, count, jnp.where(place == source, 0, -count - 1))
        fresh = jnp.where(pos <= tokpos + ahead, fresh, NEG)
        s_new[turn] = fresh
        score = jnp.dot(q, ke[...], preferred_element_type=f32)
        s_low[...] = score
        peak = jnp.maximum(
            jnp.max(score, axis=1, keepdims=True),
            jnp.max(jnp.where(low, fresh, NEG), axis=1, keepdims=True),
        )
        tops[turn] = jnp.broadcast_to(peak, (rows, pair))

    score_even(0, 0)

    @pl.loop(0, n)
    def _(k):
        turn = lax.rem(k, 2)
        score = jnp.dot(qbuf[k], ko[...], preferred_element_type=f32)
        s_high[...] = score
        m_e = tops[turn]
        p_e = jnp.exp2((s_low[...] - m_e[:, 0:1]) * LOG2E).astype(bf)
        half_acc[...] = jnp.dot(p_e, ve[...], preferred_element_type=f32)
        m_o = jnp.maximum(
            jnp.max(score, axis=1, keepdims=True),
            jnp.max(jnp.where(low, NEG, s_new[turn]), axis=1, keepdims=True),
        )
        both = jnp.where(low, m_e, m_o)
        level[...] = both
        p_new[...] = jnp.exp2((s_new[turn] - both) * LOG2E).astype(bf)

        @pl.when(k + 1 < n)
        def _():
            remote(
                qbuf.at[k + 1], qbuf.at[k + 1], q_send.at[k + 1], q_recv.at[k + 1], {"ctx": right}
            ).wait_recv()

            @pl.when(k + 3 < n)
            def _():
                onward = lax.rem(place + n + 1 - 2 * lax.rem(k, 2), n)
                remote(
                    qbuf.at[k + 1],
                    qbuf.at[k + 3],
                    q_send.at[k + 3],
                    q_recv.at[k + 3],
                    {"ctx": onward},
                ).start()

        score_even(jnp.minimum(k + 1, n - 1), 1 - turn)
        both = level[...]
        p_o = jnp.exp2((s_high[...] - both[:, half : half + 1]) * LOG2E).astype(bf)
        whole = (
            half_acc[...]
            + jnp.dot(p_o, vo[...], preferred_element_type=f32)
            + jnp.dot(p_new[...], vn[...], preferred_element_type=f32)
        )
        num = whole[:, 0:pair]
        tot = whole[:, pair : 2 * pair]
        obuf[k] = (num / tot).astype(bf)
        turned = (both + jnp.log(tot)).T
        first = lax.broadcasted_iota(jnp.int32, (8, rows), 0) < 4
        lbuf[k] = jnp.where(first, turned[0:8, :], turned[half : half + 8, :])

        @pl.when(k > 0)
        def _():
            there = {"ctx": source_of(k)}
            remote(obuf.at[k], rbuf_o.at[k], o_send.at[k], o_recv.at[k], there).start()
            remote(lbuf.at[k], rlse.at[k], l_send.at[k], l_recv.at[k], there).start()

    for i in range(heads):

        @pl.when(h == i)
        def _():
            own[...] = tok[:, i * width : (i + 1) * width].astype(f32)
            gain[...] = gain_ref[:, i * width : (i + 1) * width]

    ids = ids_ref[...]
    given = weights_ref[...]
    index = lax.broadcasted_iota(jnp.int32, (count, experts), 1)
    named = jnp.zeros((count, experts), f32)
    amount = jnp.zeros((count, experts), f32)
    for j in range(ids.shape[1]):
        hit = ids[:, j : j + 1] == index
        named = named + jnp.where(hit, 1.0, 0.0)
        amount = amount + jnp.where(hit, given[:, j : j + 1], 0.0)
    before = jnp.where(
        lax.broadcasted_iota(jnp.int32, (count, count), 1)
        < lax.broadcasted_iota(jnp.int32, (count, count), 0),
        1.0,
        0.0,
    ).astype(bf)
    rank = jnp.dot(before, named.astype(bf), preferred_element_type=f32)
    key = jnp.where(named > 0.5, rank, 128.0)
    spread = jnp.where(
        lax.div(lax.broadcasted_iota(jnp.int32, (experts, experts * CAP), 1), CAP)
        == lax.broadcasted_iota(jnp.int32, (experts, experts * CAP), 0),
        1.0,
        0.0,
    ).astype(bf)
    key = jnp.dot(key.astype(bf), spread, preferred_element_type=f32)
    slot = lax.rem(lax.broadcasted_iota(jnp.int32, (count, experts * CAP), 1), CAP).astype(f32)
    chosen = key == slot
    select_s[...] = jnp.where(chosen, 1.0, 0.0).T.astype(bf)

    def pieces(x):
        one = x.astype(bf)
        rest = x - one.astype(f32)
        two = rest.astype(bf)
        return one, two, (rest - two.astype(f32)).astype(bf)

    for i, piece in enumerate(pieces(amount)):
        on_slots = jnp.dot(piece, spread, preferred_element_type=f32)
        factor_s[i] = jnp.where(chosen, on_slots, 0.0).astype(bf)

    for load in loads:
        load.wait()
    tail = jnp.zeros((width, padded - width), bf)
    foot = jnp.zeros((padded - width, padded), bf)
    for i in range(heads):
        for j in range(2):
            wgu[i, j * padded : j * padded + width, :] = jnp.concatenate(
                [raw[j, :, i * width : (i + 1) * width], tail], axis=1
            )
            wgu[i, j * padded + width : (j + 1) * padded, :] = foot
        wdn[i, 0:width, :] = jnp.concatenate([raw[2, :, i * width : (i + 1) * width], tail], axis=1)
        wdn[i, width:padded, :] = foot
    wo_copy.wait()

    @pl.loop(1, n)
    def _(k):
        here = {"ctx": right}
        remote(obuf.at[k], rbuf_o.at[k], o_send.at[k], o_recv.at[k], here).wait_recv()
        remote(lbuf.at[k], rlse.at[k], l_send.at[k], l_recv.at[k], here).wait_recv()

    rbuf_o[0] = obuf[0]
    rlse[0] = lbuf[0]
    lse = [rlse[k] for k in range(n)]
    peak = lse[0]
    for k in range(1, n):
        peak = jnp.maximum(peak, lse[k])
    parts = [jnp.exp(x - peak) for x in lse]
    whole = parts[0]
    for k in range(1, n):
        whole = whole + parts[k]
    share = jnp.concatenate([x / whole for x in parts], axis=0)
    share = jnp.concatenate([share, share], axis=0).T
    upper = share.astype(bf).astype(f32)
    first = lax.broadcasted_iota(jnp.int32, share.shape, 1) < 8 * n
    split = jnp.where(first, upper, share - upper).astype(bf)
    spot = lax.broadcasted_iota(jnp.int32, (16 * n, pair * n), 1)
    line = lax.broadcasted_iota(jnp.int32, (16 * n, pair * n), 0)
    wanted = lax.div(spot, pair) * 8 + jnp.where(lax.rem(spot, pair) < half, 0, 4)
    pick = jnp.where(lax.rem(line, 8 * n) == wanted, 1.0, 0.0).astype(bf)
    factor = jnp.dot(split, pick, preferred_element_type=f32)
    attn = jnp.zeros((rows, pair), f32)
    for k in range(n):
        attn = attn + factor[:, pair * k : pair * (k + 1)] * rbuf_o[k].astype(f32)
    attn = attn.astype(bf)
    flat = jnp.concatenate([attn[count * j : count * (j + 1), :] for j in range(rows // count)], axis=1)

    @pl.loop(0, heads - 1)
    def _(i):
        there = lax.rem(lane_of + 1 + i, heads)
        part = lax.dot_general(flat, wo[there], NT, preferred_element_type=f32)
        pbuf[i] = part.astype(bf)
        remote(pbuf.at[i], prec.at[i], p_send.at[i], p_recv.at[i], {"head": there}).start()

    mine = lax.dot_general(flat, wo[lane_of], NT, preferred_element_type=f32)
    total = own[...] + mine
    for i in range(heads - 1):
        there = lax.rem(lane_of + 1 + i, heads)
        remote(pbuf.at[i], prec.at[i], p_send.at[i], p_recv.at[i], {"head": there}).wait_recv()
        total = total + prec[i].astype(f32)
    resid_s[...] = total

    resid = resid_s[...]
    wide[...] = jnp.zeros(wide.shape, f32)
    wide[:, 0:width] = resid * gain[...]
    power = jnp.sum(resid * resid, axis=1, keepdims=True)
    lane = lax.broadcasted_iota(jnp.int32, (count, padded), 1)
    row = wide[...]
    for i, piece in enumerate(pieces(power)):
        row = jnp.where(lane == width + i, piece.astype(f32), row)
    packed[...] = jnp.dot(select_s[...], row.astype(bf), preferred_element_type=f32).astype(bf)

    me = s * ctxs + c
    mine = pl.ds(pl.multiple_of(me * CAP, CAP), CAP)

    @pl.loop(1, experts)
    def _(step):
        s_to = lax.rem(s + seqs - lax.div(step, ctxs), seqs)
        c_to = lax.rem(c + lax.rem(step, ctxs), ctxs)
        at = pl.ds(pl.multiple_of((s_to * ctxs + c_to) * CAP, CAP), CAP)
        remote(
            packed.at[at], xall.at[0, mine], d_send.at[step], d_recv.at[step], {"seq": s_to, "ctx": c_to}
        ).start()

    xall[0, mine] = packed[mine]

    def rows_of(g):
        return pl.ds(pl.multiple_of(lax.rem(s + g, seqs) * block, block), block)

    def gather(kind, g, source, target):
        at = rows_of(g)
        return remote(
            xall.at[source, at],
            xall.at[kind, at],
            g_send.at[kind, g],
            g_recv.at[kind, g],
            {"head": target},
        )

    def stage_a(g):
        @pl.loop(1 if g == 0 else 0, ctxs)
        def _(dc):
            step = g * ctxs + dc
            at = pl.ds(0, CAP)
            remote(
                packed.at[at], xall.at[0, mine], d_send.at[step], d_recv.at[step], {"ctx": lax.rem(c + 1, ctxs)}
            ).wait_recv()

        gather(1, g, 0, other).start()
        gather(2, g, 0, above).start()
        gather(3, g, 0, below).start()

    def stage_b(g):
        gather(1, g, 0, other).wait_recv()
        gather(4, g, 1, above).start()
        gather(5, g, 1, below).start()
        gather(2, g, 0, above).wait_recv()
        gather(3, g, 0, below).wait_recv()
        if g % 2 == 0:
            gather(6, g, 2, above).start()
        else:
            gather(6, g, 3, below).start()

    def stage_c(g):
        gather(6, g, 2, above).wait_recv()
        gather(7, g, 6, other).start()

    slabs = [h, other, below, above, head_at(1, -1), head_at(1, 1), head_at(0, 2), head_at(1, 2)]

    def absorb(low, high):
        @pl.loop(low, high)
        def _(kind):
            where = slabs[low]
            for k in range(low + 1, high):
                where = jnp.where(kind == k, slabs[k], where)
            update = lax.dot_general(xall[kind], wgu[where], NT, preferred_element_type=f32)
            if low == 0:
                acc[...] = update
            else:
                acc[...] += update

    stage_a(0)
    stage_a(1)
    stage_b(0)
    stage_a(2)
    stage_b(1)
    stage_c(0)
    stage_a(3)
    stage_b(2)
    stage_c(1)
    absorb(0, 1)
    stage_b(3)
    stage_c(2)
    absorb(1, 4)
    stage_c(3)
    for g in range(GROUPS):
        gather(4, g, 1, above).wait_recv()
        gather(5, g, 1, below).wait_recv()
    absorb(4, 7)
    for g in range(GROUPS):
        gather(7, g, 6, other).wait_recv()
    absorb(7, 8)

    @pl.loop(0, GROUPS)
    def _(g):
        at = pl.ds(pl.multiple_of(g * block, block), block)
        tile = jnp.zeros((block, 128), f32)
        for k in range(heads):
            tile = tile + xall[k, at, padded - 128 : padded].astype(f32)
        spot = lax.broadcasted_iota(jnp.int32, (block, 128), 1) + (padded - 128)
        tile = jnp.where((spot >= width) & (spot < width + 3), tile, 0.0)
        power = jnp.sum(tile, axis=1, keepdims=True)
        scale = lax.rsqrt(power / (width * heads) + 1e-05)
        gate = acc[at, 0:padded] * scale
        up = acc[at, padded : 2 * padded] * scale
        hidden[at] = (gate * jax.nn.sigmoid(1.702 * gate) * (up + 1.0)).astype(bf)

    def part(g, target):
        return jnp.dot(hidden[rows_of(g)], wdn[target], preferred_element_type=f32)

    def scatter(kind, g, target):
        return remote(
            sbuf.at[kind, g], rbuf.at[kind, g], s_send.at[kind, g], s_recv.at[kind, g], {"head": target}
        )

    def got(kind, g):
        scatter(kind, g, other).wait_recv()
        return rbuf[kind, g].astype(f32)

    def send(kind, g, value, target):
        sbuf[kind, g] = value.astype(bf)
        scatter(kind, g, target).start()

    @pl.loop(0, GROUPS + 4)
    def _(t):
        @pl.when(t < GROUPS)
        def _():
            g = t
            even = lax.rem(g, 2) == 0
            send(0, g, part(g, head_at(1, 2)), other)
            send(1, g, part(g, head_at(1, -1)), below)
            send(2, g, part(g, head_at(1, 1)), above)

            @pl.when(even)
            def _():
                send(5, g, part(g, below), below)

            @pl.when(jnp.logical_not(even))
            def _():
                send(6, g, part(g, above), above)

        @pl.when((t >= 2) & (t < GROUPS + 2))
        def _():
            g = t - 2
            even = lax.rem(g, 2) == 0
            value = part(g, head_at(0, 2)) + got(0, g)
            send(3, g, value, jnp.where(even, above, below))
            value = part(g, other) + got(1, g) + got(2, g)
            send(4, g, value, other)

        @pl.when((t >= 3) & (t < GROUPS + 3))
        def _():
            g = t - 3
            even = lax.rem(g, 2) == 0

            @pl.when(even)
            def _():
                send(6, g, part(g, above) + got(3, g), above)

            @pl.when(jnp.logical_not(even))
            def _():
                send(5, g, part(g, below) + got(3, g), below)

        @pl.when(t >= 4)
        def _():
            g = t - 4
            value = part(g, h) + got(4, g) + got(5, g) + got(6, g)
            final[rows_of(g)] = value.astype(bf)
            s_to = lax.rem(s + g, seqs)

            @pl.loop(0, ctxs)
            def _(dc):
                @pl.when(g * ctxs + dc > 0)
                def _():
                    step = g * ctxs + dc
                    c_to = lax.rem(c + dc, ctxs)
                    at = pl.ds(pl.multiple_of((s_to * ctxs + c_to) * CAP, CAP), CAP)
                    remote(
                        final.at[at], back.at[mine], b_send.at[step], b_recv.at[step], {"seq": s_to, "ctx": c_to}
                    ).start()

    back[mine] = final[mine]

    def returned(step):
        at = pl.ds(0, CAP)
        return remote(
            final.at[at], back.at[mine], b_send.at[step], b_recv.at[step], {"ctx": lax.rem(c + 1, ctxs)}
        )

    @pl.loop(1, experts)
    def _(step):
        returned(step).wait_recv()

    moe = jnp.zeros((count, padded), f32)
    for i in range(3):
        moe = moe + jnp.dot(factor_s[i], back[...], preferred_element_type=f32)
    out_ref[...] = (resid_s[...] + moe[:, 0:width]).astype(bf)

    @pl.loop(1, experts)
    def _(step):
        at = pl.ds(0, CAP)
        remote(
            packed.at[at], xall.at[0, mine], d_send.at[step], d_recv.at[step], {"ctx": lax.rem(c + 1, ctxs)}
        ).wait_send()
        returned(step).wait_send()

    for g in range(GROUPS):
        for kind in range(1, heads):
            gather(kind, g, 0, other).wait_send()
        for kind in range(heads - 1):
            scatter(kind, g, other).wait_send()

    @pl.loop(1, n)
    def _(k):
        here = {"ctx": right}
        remote(qbuf.at[k], qbuf.at[k], q_send.at[k], q_recv.at[k], here).wait_send()
        remote(obuf.at[k], rbuf_o.at[k], o_send.at[k], o_recv.at[k], here).wait_send()
        remote(lbuf.at[k], rlse.at[k], l_send.at[k], l_recv.at[k], here).wait_send()

    @pl.loop(0, heads - 1)
    def _(c):
        there = lax.rem(lane_of + 1 + c, heads)
        remote(pbuf.at[c], prec.at[c], p_send.at[c], p_recv.at[c], {"head": there}).wait_send()


def layer(tokens, qw, kt, vt, nk, nv, wo, gain, ids, weights, gate, up, down):
    seqs, ctxs, heads = lax.axis_size("seq"), lax.axis_size("ctx"), lax.axis_size("head")
    experts = seqs * ctxs
    slots = experts * CAP
    count, model = tokens.shape
    width = model // heads
    half, cached = kt.shape
    pair = 2 * half
    rows = qw.shape[1] // pair * count
    hidden = gate.shape[0]
    padded = -(-(width + 3) // 128) * 128
    block = ctxs * CAP
    bf, f32 = jnp.bfloat16, jnp.float32
    vm = pl.BlockSpec(memory_space=pltpu.VMEM)
    hbm = pl.BlockSpec(memory_space=pl.ANY)
    dma = pltpu.SemaphoreType.DMA
    spans = -(-model // DEPTH)
    return pl.pallas_call(
        layer_kernel,
        out_shape=jax.ShapeDtypeStruct((count, width), bf),
        in_specs=[hbm] * 4 + [vm] * 2 + [hbm] + [vm] * 3 + [hbm] * 3,
        out_specs=vm,
        scratch_shapes=[
            pltpu.VMEM((count, model), bf),
            pltpu.VMEM(qw.shape, bf),
            pltpu.VMEM(vt.shape, bf),
            pltpu.VMEM((count, width), f32),
            pltpu.VMEM((1, width), f32),
            pltpu.VMEM((count, width), f32),
            pltpu.VMEM((ctxs, rows, pair), bf),
            pltpu.VMEM((pair, cached), bf),
            pltpu.VMEM((pair, cached), bf),
            pltpu.VMEM((cached, 2 * pair), bf),
            pltpu.VMEM((cached, 2 * pair), bf),
            pltpu.VMEM((2 * count, pair), bf),
            pltpu.VMEM((2 * count, 2 * pair), bf),
            pltpu.VMEM((rows, cached), f32),
            pltpu.VMEM((rows, cached), f32),
            pltpu.VMEM((2, rows, pair), f32),
            pltpu.VMEM((2, rows, pair), f32),
            pltpu.VMEM((rows, pair), f32),
            pltpu.VMEM((rows, pair), bf),
            pltpu.VMEM((rows, 2 * pair), f32),
            pltpu.VMEM((ctxs, rows, pair), bf),
            pltpu.VMEM((ctxs, 8, rows), f32),
            pltpu.VMEM((ctxs, rows, pair), bf),
            pltpu.VMEM((ctxs, 8, rows), f32),
            pltpu.VMEM(wo.shape, bf),
            pltpu.VMEM((heads - 1, count, width), bf),
            pltpu.VMEM((heads - 1, count, width), bf),
            pltpu.VMEM((3, hidden, model), bf),
            pltpu.VMEM((count, padded), f32),
            pltpu.VMEM((heads, 2 * padded, padded), bf),
            pltpu.VMEM((heads, padded, padded), bf),
            pltpu.VMEM((slots, count), bf),
            pltpu.VMEM((3, count, slots), bf),
            pltpu.VMEM((slots, padded), bf),
            pltpu.VMEM((heads, slots, padded), bf),
            pltpu.VMEM((slots, 2 * padded), f32),
            pltpu.VMEM((slots, padded), bf),
            pltpu.VMEM((heads - 1, GROUPS, block, padded), bf),
            pltpu.VMEM((heads - 1, GROUPS, block, padded), bf),
            pltpu.VMEM((slots, padded), bf),
            pltpu.VMEM((slots, padded), bf),
            dma((4 + spans,)),
            dma((ctxs,)),
            dma((ctxs,)),
            dma((ctxs,)),
            dma((ctxs,)),
            dma((ctxs,)),
            dma((ctxs,)),
            dma((heads - 1,)),
            dma((heads - 1,)),
            dma((4,)),
            dma((experts,)),
            dma((experts,)),
            dma((heads, GROUPS)),
            dma((heads, GROUPS)),
            dma((heads - 1, GROUPS)),
            dma((heads - 1, GROUPS)),
            dma((experts,)),
            dma((experts,)),
        ],
        compiler_params=pltpu.CompilerParams(
            collective_id=0, has_side_effects=True, vmem_limit_bytes=60 * 1024 * 1024
        ),
    )(tokens, qw, kt, vt, nk, nv, wo, gain, ids, weights, gate, up, down)


def body(
    stream,
    query_weight,
    cache_keys,
    cache_values,
    new_keys,
    new_values,
    out_weight,
    norm_gain,
    expert_ids,
    expert_weights,
    gate_weight,
    up_weight,
    down_weight,
):
    heads = lax.axis_size("head")
    taken, model = out_weight.shape
    mixed = layer(
        stream[0],
        query_weight,
        cache_keys[0, :, 0, :].T,
        cache_values[0, :, 0, :].T,
        new_keys[0, :, 0, :],
        new_values[0, :, 0, :],
        out_weight.T.reshape(heads, model // heads, taken),
        norm_gain[None],
        expert_ids[0],
        expert_weights[0],
        gate_weight[0].T,
        up_weight[0].T,
        down_weight[0],
    )
    return mixed[None]


def solution(mesh):
    in_specs = (
        P("seq", "ctx", None),
        P(None, "head"),
        P("seq", "ctx", "head", None),
        P("seq", "ctx", "head", None),
        P("seq", "ctx", "head", None),
        P("seq", "ctx", "head", None),
        P("head", None),
        P(),
        P("seq", "ctx", None),
        P("seq", "ctx", None),
        P(("seq", "ctx"), None, "head"),
        P(("seq", "ctx"), None, "head"),
        P(("seq", "ctx"), "head", None),
    )
    out_specs = P("seq", "ctx", "head")
    return jax.shard_map(body, mesh=mesh, in_specs=in_specs, out_specs=out_specs, check_vma=False)
```

```python
import math

import jax
import jax.numpy as jnp
from jax import lax
from jax.experimental import pallas as pl
from jax.experimental.pallas import tpu as pltpu
from jax.sharding import PartitionSpec as P

CAP = 16
MESH = pl.DeviceIdType.MESH
LOG2E = 1.4426950408889634
NEG = -3.0e38
NT = (((1,), (1,)), ((), ()))
GROUPS = 4
DEPTH = 768


def remote(src, dst, send, recv, where):
    return pltpu.make_async_remote_copy(
        src_ref=src, dst_ref=dst, send_sem=send, recv_sem=recv, device_id=where, device_id_type=MESH
    )


def layer_kernel(
    tok_hbm,
    qw_hbm,
    kt_hbm,
    vt_hbm,
    nk_hbm,
    nv_hbm,
    wo_hbm,
    gain_hbm,
    ids_hbm,
    weights_hbm,
    gate_hbm,
    up_hbm,
    down_hbm,
    out_ref,
    nk_ref,
    nv_ref,
    gain_ref,
    ids_ref,
    weights_ref,
    tok,
    qw,
    vt,
    own,
    gain,
    resid_s,
    qbuf,
    ke,
    ko,
    ve,
    vo,
    kn,
    vn,
    s_low,
    s_high,
    s_new,
    tops,
    level,
    p_new,
    half_acc,
    obuf,
    lbuf,
    rbuf_o,
    rlse,
    wo,
    pbuf,
    prec,
    raw,
    wide,
    wgu,
    wdn,
    select_s,
    factor_s,
    packed,
    xall,
    acc,
    hidden,
    sbuf,
    rbuf,
    final,
    back,
    in_sem,
    e_sem,
    q_send,
    q_recv,
    o_send,
    o_recv,
    l_send,
    l_recv,
    p_send,
    p_recv,
    w_sem,
    d_send,
    d_recv,
    g_send,
    g_recv,
    s_send,
    s_recv,
    b_send,
    b_recv,
):
    seqs, ctxs, heads = lax.axis_size("seq"), lax.axis_size("ctx"), lax.axis_size("head")
    s, c, h = lax.axis_index("seq"), lax.axis_index("ctx"), lax.axis_index("head")
    n, place, lane_of = ctxs, c, h
    experts = seqs * ctxs
    count, model = tok.shape
    width = own.shape[1]
    padded = wide.shape[1]
    block = ctxs * CAP
    f32, bf = jnp.float32, jnp.bfloat16
    ring = heads // 2
    col, y = lax.div(h, ring), lax.rem(h, ring)
    rows = qbuf.shape[1]
    half = ke.shape[0] // 2
    cached = ke.shape[1]
    pair = 2 * half

    def head_at(across, dy):
        return (col if across == 0 else 1 - col) * ring + lax.rem(y + dy + ring, ring)

    other, above, below = head_at(1, 0), head_at(0, 1), head_at(0, -1)
    edges = list(range(0, model, DEPTH)) + [model]
    spans = list(zip(edges[:-1], edges[1:]))
    tok_load = pltpu.make_async_copy(tok_hbm, tok, in_sem.at[0])
    qw_loads = [
        pltpu.make_async_copy(qw_hbm.at[low:high], qw.at[low:high], in_sem.at[4 + i])
        for i, (low, high) in enumerate(spans)
    ]
    kv_loads = [
        pltpu.make_async_copy(kt_hbm, ke.at[0:half], in_sem.at[1]),
        pltpu.make_async_copy(kt_hbm, ko.at[half:pair], in_sem.at[2]),
        pltpu.make_async_copy(vt_hbm, vt, in_sem.at[3]),
    ]
    small = [
        pltpu.make_async_copy(source, target, e_sem.at[i])
        for i, (source, target) in enumerate(
            (
                (nk_hbm, nk_ref),
                (nv_hbm, nv_ref),
                (gain_hbm, gain_ref),
                (ids_hbm, ids_ref),
                (weights_hbm, weights_ref),
            )
        )
    ]
    for load in [tok_load] + qw_loads + kv_loads + small:
        load.start()
    wo_copy = pltpu.make_async_copy(wo_hbm, wo, w_sem.at[3])
    loads = [
        pltpu.make_async_copy(source, raw.at[i], w_sem.at[i])
        for i, source in enumerate((gate_hbm, up_hbm, down_hbm))
    ]
    barrier = pltpu.get_barrier_semaphore()

    @pl.loop(1, experts)
    def _(step):
        there = {
            "seq": lax.rem(s + lax.div(step, ctxs), seqs),
            "ctx": lax.rem(c + lax.rem(step, ctxs), ctxs),
        }
        pl.semaphore_signal(barrier, inc=1, device_id=there, device_id_type=MESH)

    @pl.loop(1, heads)
    def _(step):
        there = {"head": lax.rem(h + step, heads)}
        pl.semaphore_signal(barrier, inc=1, device_id=there, device_id_type=MESH)

    ke[half:pair, :] = jnp.zeros((half, cached), bf)
    ko[0:half, :] = jnp.zeros((half, cached), bf)
    tok_load.wait()
    query = jnp.zeros((count, qw.shape[1]), f32)
    for (low_k, high_k), load in zip(spans, qw_loads):
        load.wait()
        query = query + jnp.dot(tok[:, low_k:high_k], qw[low_k:high_k, :], preferred_element_type=f32)
    query = (query.astype(bf).astype(f32) * (1.0 / math.sqrt(half))).astype(bf)
    for j in range(rows // count):
        qbuf[0, count * j : count * (j + 1), :] = query[:, pair * j : pair * (j + 1)]
    for load in kv_loads + small:
        load.wait()
    low_n = lax.broadcasted_iota(jnp.int32, (count, pair), 1) < half
    nk = nk_ref[...].astype(f32)
    nk = jnp.concatenate([nk, nk], axis=1)
    nv = nv_ref[...].astype(f32)
    nv = jnp.concatenate([nv, nv], axis=1)
    kn[0:count, :] = jnp.where(low_n, nk, 0.0).astype(bf)
    kn[count : 2 * count, :] = jnp.where(low_n, 0.0, nk).astype(bf)
    vn[0:count, 0:pair] = jnp.where(low_n, nv, 0.0).astype(bf)
    vn[count : 2 * count, 0:pair] = jnp.where(low_n, 0.0, nv).astype(bf)
    vn[0:count, pair : 2 * pair] = jnp.where(low_n, 1.0, 0.0).astype(bf)
    vn[count : 2 * count, pair : 2 * pair] = jnp.where(low_n, 0.0, 1.0).astype(bf)

    pl.semaphore_wait(barrier, experts - 1 + heads - 1)
    right = lax.rem(place + 1, n)
    left = lax.rem(place + n - 1, n)
    remote(qbuf.at[0], qbuf.at[1], q_send.at[1], q_recv.at[1], {"ctx": right}).start()
    remote(qbuf.at[0], qbuf.at[2], q_send.at[2], q_recv.at[2], {"ctx": left}).start()
    wo_copy.start()
    for load in loads:
        load.start()

    span = 256

    @pl.loop(0, cached // span)
    def _(i):
        at = pl.ds(pl.multiple_of(i * span, span), span)
        ones = jnp.where(lax.broadcasted_iota(jnp.int32, (span, pair), 1) < half, 1.0, 0.0)
        v = vt[:, at].astype(f32)
        blank = jnp.zeros_like(v)
        ve[at, 0:pair] = jnp.concatenate([v, blank], 0).T.astype(bf)
        vo[at, 0:pair] = jnp.concatenate([blank, v], 0).T.astype(bf)
        ve[at, pair : 2 * pair] = ones.astype(bf)
        vo[at, pair : 2 * pair] = (1.0 - ones).astype(bf)

    lane = lax.broadcasted_iota(jnp.int32, (rows, pair), 1)
    low = lane < half
    tokpos = lax.rem(lax.broadcasted_iota(jnp.int32, (rows, pair), 0), count)
    pos = lax.rem(lane, half)

    def source_of(k):
        return lax.rem(place + lax.div(k + 1, 2) * (1 - 2 * lax.rem(k, 2)) + n, n)

    def score_even(k, turn):
        q = qbuf[k]
        source = source_of(k)
        fresh = lax.dot_general(q, kn[...], NT, preferred_element_type=f32)
        ahead = jnp.where(place < source, count, jnp.where(place == source, 0, -count - 1))
        fresh = jnp.where(pos <= tokpos + ahead, fresh, NEG)
        s_new[turn] = fresh
        score = jnp.dot(q, ke[...], preferred_element_type=f32)
        s_low[...] = score
        peak = jnp.maximum(
            jnp.max(score, axis=1, keepdims=True),
            jnp.max(jnp.where(low, fresh, NEG), axis=1, keepdims=True),
        )
        tops[turn] = jnp.broadcast_to(peak, (rows, pair))

    score_even(0, 0)

    @pl.loop(0, n)
    def _(k):
        turn = lax.rem(k, 2)
        score = jnp.dot(qbuf[k], ko[...], preferred_element_type=f32)
        s_high[...] = score
        m_e = tops[turn]
        p_e = jnp.exp2((s_low[...] - m_e[:, 0:1]) * LOG2E).astype(bf)
        half_acc[...] = jnp.dot(p_e, ve[...], preferred_element_type=f32)
        m_o = jnp.maximum(
            jnp.max(score, axis=1, keepdims=True),
            jnp.max(jnp.where(low, NEG, s_new[turn]), axis=1, keepdims=True),
        )
        both = jnp.where(low, m_e, m_o)
        level[...] = both
        p_new[...] = jnp.exp2((s_new[turn] - both) * LOG2E).astype(bf)

        @pl.when(k + 1 < n)
        def _():
            remote(
                qbuf.at[k + 1], qbuf.at[k + 1], q_send.at[k + 1], q_recv.at[k + 1], {"ctx": right}
            ).wait_recv()

            @pl.when(k + 3 < n)
            def _():
                onward = lax.rem(place + n + 1 - 2 * lax.rem(k, 2), n)
                remote(
                    qbuf.at[k + 1],
                    qbuf.at[k + 3],
                    q_send.at[k + 3],
                    q_recv.at[k + 3],
                    {"ctx": onward},
                ).start()

        score_even(jnp.minimum(k + 1, n - 1), 1 - turn)
        both = level[...]
        p_o = jnp.exp2((s_high[...] - both[:, half : half + 1]) * LOG2E).astype(bf)
        whole = (
            half_acc[...]
            + jnp.dot(p_o, vo[...], preferred_element_type=f32)
            + jnp.dot(p_new[...], vn[...], preferred_element_type=f32)
        )
        num = whole[:, 0:pair]
        tot = whole[:, pair : 2 * pair]
        obuf[k] = (num / tot).astype(bf)
        turned = (both + jnp.log(tot)).T
        for i in range(2):
            for j in range(2):
                lbuf[k, 2 * i + j : 2 * i + j + 1, :] = turned[i * half : i * half + 1, j * pair : (j + 1) * pair]

        @pl.when(k > 0)
        def _():
            there = {"ctx": source_of(k)}
            remote(obuf.at[k], rbuf_o.at[k], o_send.at[k], o_recv.at[k], there).start()
            remote(lbuf.at[k], rlse.at[k], l_send.at[k], l_recv.at[k], there).start()

    for i in range(heads):

        @pl.when(h == i)
        def _():
            own[...] = tok[:, i * width : (i + 1) * width].astype(f32)
            gain[...] = gain_ref[i * width : (i + 1) * width].reshape(1, width)

    ids = ids_ref[...]
    given = weights_ref[...]
    index = lax.broadcasted_iota(jnp.int32, (experts, count), 0)
    named = jnp.zeros((experts, count), f32)
    amount = jnp.zeros((experts, count), f32)
    for j in range(ids.shape[0]):
        hit = ids[j : j + 1, :] == index
        named = named + jnp.where(hit, 1.0, 0.0)
        amount = amount + jnp.where(hit, given[j : j + 1, :], 0.0)
    before = jnp.where(
        lax.broadcasted_iota(jnp.int32, (count, count), 0)
        < lax.broadcasted_iota(jnp.int32, (count, count), 1),
        1.0,
        0.0,
    ).astype(bf)
    rank = jnp.dot(named.astype(bf), before, preferred_element_type=f32)
    key = jnp.where(named > 0.5, rank, 128.0)
    spread = jnp.where(
        lax.div(lax.broadcasted_iota(jnp.int32, (experts * CAP, experts), 0), CAP)
        == lax.broadcasted_iota(jnp.int32, (experts * CAP, experts), 1),
        1.0,
        0.0,
    ).astype(bf)
    key = jnp.dot(spread, key.astype(bf), preferred_element_type=f32)
    slot = lax.rem(lax.broadcasted_iota(jnp.int32, (experts * CAP, count), 0), CAP).astype(f32)
    chosen = key == slot
    select_s[...] = jnp.where(chosen, 1.0, 0.0).astype(bf)

    def pieces(x):
        one = x.astype(bf)
        rest = x - one.astype(f32)
        two = rest.astype(bf)
        return one, two, (rest - two.astype(f32)).astype(bf)

    for i, piece in enumerate(pieces(amount)):
        on_slots = jnp.dot(spread, piece, preferred_element_type=f32)
        factor_s[i] = jnp.where(chosen, on_slots, 0.0).T.astype(bf)

    for load in loads:
        load.wait()
    tail = jnp.zeros((width, padded - width), bf)
    foot = jnp.zeros((padded - width, padded), bf)
    for i in range(heads):
        for j in range(2):
            wgu[i, j * padded : j * padded + width, :] = jnp.concatenate(
                [raw[j, :, i * width : (i + 1) * width], tail], axis=1
            )
            wgu[i, j * padded + width : (j + 1) * padded, :] = foot
        wdn[i, 0:width, :] = jnp.concatenate([raw[2, :, i * width : (i + 1) * width], tail], axis=1)
        wdn[i, width:padded, :] = foot
    wo_copy.wait()

    @pl.loop(1, n)
    def _(k):
        here = {"ctx": right}
        remote(obuf.at[k], rbuf_o.at[k], o_send.at[k], o_recv.at[k], here).wait_recv()
        remote(lbuf.at[k], rlse.at[k], l_send.at[k], l_recv.at[k], here).wait_recv()

    rbuf_o[0] = obuf[0]
    rlse[0] = lbuf[0]
    lse = [rlse[k] for k in range(n)]
    peak = lse[0]
    for k in range(1, n):
        peak = jnp.maximum(peak, lse[k])
    parts = [jnp.exp(x - peak) for x in lse]
    whole = parts[0]
    for k in range(1, n):
        whole = whole + parts[k]
    share = jnp.concatenate([x / whole for x in parts], axis=0)
    share = jnp.concatenate([share, share], axis=0).T
    upper = share.astype(bf).astype(f32)
    first = lax.broadcasted_iota(jnp.int32, share.shape, 1) < 4 * n
    split = jnp.where(first, upper, share - upper).astype(bf)
    spot = lax.broadcasted_iota(jnp.int32, (8 * n, pair * n), 1)
    line = lax.rem(lax.broadcasted_iota(jnp.int32, (8 * n, pair * n), 0), 4 * n)
    wanted = lax.div(spot, pair) * 4 + jnp.where(lax.rem(spot, pair) < half, 0, 2)
    halves = []
    for j in range(2):
        pick = jnp.where(line == wanted + j, 1.0, 0.0).astype(bf)
        factor = jnp.dot(split, pick, preferred_element_type=f32)
        total = jnp.zeros((pair, pair), f32)
        for k in range(n):
            total = total + factor[:, pair * k : pair * (k + 1)] * rbuf_o[k, j * pair : (j + 1) * pair, :].astype(f32)
        halves.append(total.astype(bf))
    attn = jnp.concatenate(halves, axis=0)
    flat = jnp.concatenate([attn[count * j : count * (j + 1), :] for j in range(rows // count)], axis=1)

    def peer_at(i):
        across = jnp.where(i < ring, 1 - col, col)
        dy = jnp.where(i < ring, 2 + i, i - ring + 1)
        return across * ring + lax.rem(y + dy, ring)

    @pl.loop(0, heads - 1)
    def _(i):
        there = peer_at(i)
        part = lax.dot_general(flat, wo[there], NT, preferred_element_type=f32)
        pbuf[i] = part.astype(bf)
        remote(pbuf.at[i], prec.at[i], p_send.at[i], p_recv.at[i], {"head": there}).start()

    mine = lax.dot_general(flat, wo[lane_of], NT, preferred_element_type=f32)
    total = own[...] + mine
    for i in range(heads - 1):
        there = peer_at(i)
        remote(pbuf.at[i], prec.at[i], p_send.at[i], p_recv.at[i], {"head": there}).wait_recv()
        total = total + prec[i].astype(f32)
    resid_s[...] = total

    resid = resid_s[...]
    wide[...] = jnp.zeros(wide.shape, f32)
    wide[:, 0:width] = resid * gain[...]
    power = jnp.sum(resid * resid, axis=1, keepdims=True)
    lane = lax.broadcasted_iota(jnp.int32, (count, padded), 1)
    row = wide[...]
    for i, piece in enumerate(pieces(power)):
        row = jnp.where(lane == width + i, piece.astype(f32), row)
    packed[...] = jnp.dot(select_s[...], row.astype(bf), preferred_element_type=f32).astype(bf)

    me = s * ctxs + c
    mine = pl.ds(pl.multiple_of(me * CAP, CAP), CAP)

    @pl.loop(1, experts)
    def _(step):
        s_to = lax.rem(s + seqs - lax.div(step, ctxs), seqs)
        c_to = lax.rem(c + lax.rem(step, ctxs), ctxs)
        at = pl.ds(pl.multiple_of((s_to * ctxs + c_to) * CAP, CAP), CAP)
        remote(
            packed.at[at], xall.at[0, mine], d_send.at[step], d_recv.at[step], {"seq": s_to, "ctx": c_to}
        ).start()

    xall[0, mine] = packed[mine]

    def rows_of(g):
        return pl.ds(pl.multiple_of(lax.rem(s + g, seqs) * block, block), block)

    def gather(kind, g, source, target):
        at = rows_of(g)
        return remote(
            xall.at[source, at],
            xall.at[kind, at],
            g_send.at[kind, g],
            g_recv.at[kind, g],
            {"head": target},
        )

    def stage_a(g):
        @pl.loop(1 if g == 0 else 0, ctxs)
        def _(dc):
            step = g * ctxs + dc
            at = pl.ds(0, CAP)
            remote(
                packed.at[at], xall.at[0, mine], d_send.at[step], d_recv.at[step], {"ctx": lax.rem(c + 1, ctxs)}
            ).wait_recv()

        gather(1, g, 0, other).start()
        gather(2, g, 0, above).start()
        gather(3, g, 0, below).start()

    def stage_b(g):
        gather(1, g, 0, other).wait_recv()
        gather(4, g, 1, above).start()
        gather(5, g, 1, below).start()
        gather(2, g, 0, above).wait_recv()
        gather(3, g, 0, below).wait_recv()
        if g % 2 == 0:
            gather(6, g, 2, above).start()
        else:
            gather(6, g, 3, below).start()

    def stage_c(g):
        gather(6, g, 2, above).wait_recv()
        gather(7, g, 6, other).start()

    slabs = [h, other, below, above, head_at(1, -1), head_at(1, 1), head_at(0, 2), head_at(1, 2)]

    def absorb(low, high):
        @pl.loop(low, high)
        def _(kind):
            where = slabs[low]
            for k in range(low + 1, high):
                where = jnp.where(kind == k, slabs[k], where)
            update = lax.dot_general(xall[kind], wgu[where], NT, preferred_element_type=f32)
            if low == 0:
                acc[...] = update
            else:
                acc[...] += update

    stage_a(0)
    stage_a(1)
    stage_b(0)
    stage_a(2)
    stage_b(1)
    stage_c(0)
    stage_a(3)
    stage_b(2)
    stage_c(1)
    absorb(0, 1)
    stage_b(3)
    stage_c(2)
    absorb(1, 4)
    stage_c(3)
    for g in range(GROUPS):
        gather(4, g, 1, above).wait_recv()
        gather(5, g, 1, below).wait_recv()
    absorb(4, 7)
    for g in range(GROUPS):
        gather(7, g, 6, other).wait_recv()
    absorb(7, 8)

    @pl.loop(0, GROUPS)
    def _(g):
        at = pl.ds(pl.multiple_of(g * block, block), block)
        tile = jnp.zeros((block, 128), f32)
        for k in range(heads):
            tile = tile + xall[k, at, padded - 128 : padded].astype(f32)
        spot = lax.broadcasted_iota(jnp.int32, (block, 128), 1) + (padded - 128)
        tile = jnp.where((spot >= width) & (spot < width + 3), tile, 0.0)
        power = jnp.sum(tile, axis=1, keepdims=True)
        scale = lax.rsqrt(power / (width * heads) + 1e-05)
        gate = acc[at, 0:padded] * scale
        up = acc[at, padded : 2 * padded] * scale
        hidden[at] = (gate * jax.nn.sigmoid(1.702 * gate) * (up + 1.0)).astype(bf)

    def part(g, target):
        return jnp.dot(hidden[rows_of(g)], wdn[target], preferred_element_type=f32)

    def scatter(kind, g, target):
        return remote(
            sbuf.at[kind, g], rbuf.at[kind, g], s_send.at[kind, g], s_recv.at[kind, g], {"head": target}
        )

    def got(kind, g):
        scatter(kind, g, other).wait_recv()
        return rbuf[kind, g].astype(f32)

    def send(kind, g, value, target):
        sbuf[kind, g] = value.astype(bf)
        scatter(kind, g, target).start()

    @pl.loop(0, GROUPS + 4)
    def _(t):
        @pl.when(t < GROUPS)
        def _():
            g = t
            even = lax.rem(g, 2) == 0
            send(0, g, part(g, head_at(1, 2)), other)
            send(1, g, part(g, head_at(1, -1)), below)
            send(2, g, part(g, head_at(1, 1)), above)

            @pl.when(even)
            def _():
                send(5, g, part(g, below), below)

            @pl.when(jnp.logical_not(even))
            def _():
                send(6, g, part(g, above), above)

        @pl.when((t >= 2) & (t < GROUPS + 2))
        def _():
            g = t - 2
            even = lax.rem(g, 2) == 0
            value = part(g, head_at(0, 2)) + got(0, g)
            send(3, g, value, jnp.where(even, above, below))
            value = part(g, other) + got(1, g) + got(2, g)
            send(4, g, value, other)

        @pl.when((t >= 3) & (t < GROUPS + 3))
        def _():
            g = t - 3
            even = lax.rem(g, 2) == 0

            @pl.when(even)
            def _():
                send(6, g, part(g, above) + got(3, g), above)

            @pl.when(jnp.logical_not(even))
            def _():
                send(5, g, part(g, below) + got(3, g), below)

        @pl.when(t >= 4)
        def _():
            g = t - 4
            value = part(g, h) + got(4, g) + got(5, g) + got(6, g)
            final[rows_of(g)] = value.astype(bf)
            s_to = lax.rem(s + g, seqs)

            @pl.loop(0, ctxs)
            def _(dc):
                @pl.when(g * ctxs + dc > 0)
                def _():
                    step = g * ctxs + dc
                    c_to = lax.rem(c + dc, ctxs)
                    at = pl.ds(pl.multiple_of((s_to * ctxs + c_to) * CAP, CAP), CAP)
                    remote(
                        final.at[at], back.at[mine], b_send.at[step], b_recv.at[step], {"seq": s_to, "ctx": c_to}
                    ).start()

    back[mine] = final[mine]

    def returned(step):
        at = pl.ds(0, CAP)
        return remote(
            final.at[at], back.at[mine], b_send.at[step], b_recv.at[step], {"ctx": lax.rem(c + 1, ctxs)}
        )

    @pl.loop(1, experts)
    def _(step):
        returned(step).wait_recv()

    moe = jnp.zeros((count, padded), f32)
    for i in range(3):
        moe = moe + jnp.dot(factor_s[i], back[...], preferred_element_type=f32)
    out_ref[...] = (resid_s[...] + moe[:, 0:width]).astype(bf)

    @pl.loop(1, experts)
    def _(step):
        at = pl.ds(0, CAP)
        remote(
            packed.at[at], xall.at[0, mine], d_send.at[step], d_recv.at[step], {"ctx": lax.rem(c + 1, ctxs)}
        ).wait_send()
        returned(step).wait_send()

    for g in range(GROUPS):
        for kind in range(1, heads):
            gather(kind, g, 0, other).wait_send()
        for kind in range(heads - 1):
            scatter(kind, g, other).wait_send()

    @pl.loop(1, n)
    def _(k):
        here = {"ctx": right}
        remote(qbuf.at[k], qbuf.at[k], q_send.at[k], q_recv.at[k], here).wait_send()
        remote(obuf.at[k], rbuf_o.at[k], o_send.at[k], o_recv.at[k], here).wait_send()
        remote(lbuf.at[k], rlse.at[k], l_send.at[k], l_recv.at[k], here).wait_send()

    @pl.loop(0, heads - 1)
    def _(c):
        there = lax.rem(lane_of + 1 + c, heads)
        remote(pbuf.at[c], prec.at[c], p_send.at[c], p_recv.at[c], {"head": there}).wait_send()


def layer(tokens, qw, kt, vt, nk, nv, wo, gain, ids, weights, gate, up, down):
    seqs, ctxs, heads = lax.axis_size("seq"), lax.axis_size("ctx"), lax.axis_size("head")
    experts = seqs * ctxs
    slots = experts * CAP
    count, model = tokens.shape
    width = model // heads
    half, cached = kt.shape
    pair = 2 * half
    rows = qw.shape[1] // pair * count
    hidden = gate.shape[0]
    padded = -(-(width + 3) // 128) * 128
    block = ctxs * CAP
    bf, f32 = jnp.bfloat16, jnp.float32
    vm = pl.BlockSpec(memory_space=pltpu.VMEM)
    hbm = pl.BlockSpec(memory_space=pltpu.HBM)
    dma = pltpu.SemaphoreType.DMA
    spans = -(-model // DEPTH)
    return pl.pallas_call(
        layer_kernel,
        out_shape=jax.ShapeDtypeStruct((count, width), bf),
        in_specs=[hbm] * 13,
        out_specs=vm,
        scratch_shapes=[
            pltpu.VMEM(nk.shape, bf),
            pltpu.VMEM(nv.shape, bf),
            pltpu.VMEM(gain.shape, f32),
            pltpu.VMEM(ids.shape, jnp.int32),
            pltpu.VMEM(weights.shape, f32),
            pltpu.VMEM((count, model), bf),
            pltpu.VMEM(qw.shape, bf),
            pltpu.VMEM(vt.shape, bf),
            pltpu.VMEM((count, width), f32),
            pltpu.VMEM((1, width), f32),
            pltpu.VMEM((count, width), f32),
            pltpu.VMEM((ctxs, rows, pair), bf),
            pltpu.VMEM((pair, cached), bf),
            pltpu.VMEM((pair, cached), bf),
            pltpu.VMEM((cached, 2 * pair), bf),
            pltpu.VMEM((cached, 2 * pair), bf),
            pltpu.VMEM((2 * count, pair), bf),
            pltpu.VMEM((2 * count, 2 * pair), bf),
            pltpu.VMEM((rows, cached), f32),
            pltpu.VMEM((rows, cached), f32),
            pltpu.VMEM((2, rows, pair), f32),
            pltpu.VMEM((2, rows, pair), f32),
            pltpu.VMEM((rows, pair), f32),
            pltpu.VMEM((rows, pair), bf),
            pltpu.VMEM((rows, 2 * pair), f32),
            pltpu.VMEM((ctxs, rows, pair), bf),
            pltpu.VMEM((ctxs, 4, pair), f32),
            pltpu.VMEM((ctxs, rows, pair), bf),
            pltpu.VMEM((ctxs, 4, pair), f32),
            pltpu.VMEM(wo.shape, bf),
            pltpu.VMEM((heads - 1, count, width), bf),
            pltpu.VMEM((heads - 1, count, width), bf),
            pltpu.VMEM((3, hidden, model), bf),
            pltpu.VMEM((count, padded), f32),
            pltpu.VMEM((heads, 2 * padded, padded), bf),
            pltpu.VMEM((heads, padded, padded), bf),
            pltpu.VMEM((slots, count), bf),
            pltpu.VMEM((3, count, slots), bf),
            pltpu.VMEM((slots, padded), bf),
            pltpu.VMEM((heads, slots, padded), bf),
            pltpu.VMEM((slots, 2 * padded), f32),
            pltpu.VMEM((slots, padded), bf),
            pltpu.VMEM((heads - 1, GROUPS, block, padded), bf),
            pltpu.VMEM((heads - 1, GROUPS, block, padded), bf),
            pltpu.VMEM((slots, padded), bf),
            pltpu.VMEM((slots, padded), bf),
            dma((4 + spans,)),
            dma((5,)),
            dma((ctxs,)),
            dma((ctxs,)),
            dma((ctxs,)),
            dma((ctxs,)),
            dma((ctxs,)),
            dma((ctxs,)),
            dma((heads - 1,)),
            dma((heads - 1,)),
            dma((4,)),
            dma((experts,)),
            dma((experts,)),
            dma((heads, GROUPS)),
            dma((heads, GROUPS)),
            dma((heads - 1, GROUPS)),
            dma((heads - 1, GROUPS)),
            dma((experts,)),
            dma((experts,)),
        ],
        compiler_params=pltpu.CompilerParams(
            collective_id=0, has_side_effects=True, vmem_limit_bytes=50 * 1024 * 1024
        ),
    )(tokens, qw, kt, vt, nk, nv, wo, gain, ids, weights, gate, up, down)


def body(
    stream,
    query_weight,
    cache_keys,
    cache_values,
    new_keys,
    new_values,
    out_weight,
    norm_gain,
    expert_ids,
    expert_weights,
    gate_weight,
    up_weight,
    down_weight,
):
    heads = lax.axis_size("head")
    taken, model = out_weight.shape
    mixed = layer(
        stream[0],
        query_weight,
        cache_keys[0, :, 0, :].T,
        cache_values[0, :, 0, :].T,
        new_keys[0, :, 0, :],
        new_values[0, :, 0, :],
        out_weight.T.reshape(heads, model // heads, taken),
        norm_gain,
        expert_ids[0].T,
        expert_weights[0].T,
        gate_weight[0].T,
        up_weight[0].T,
        down_weight[0],
    )
    return mixed[None]


def solution(mesh):
    in_specs = (
        P("seq", "ctx", None),
        P(None, "head"),
        P("seq", "ctx", "head", None),
        P("seq", "ctx", "head", None),
        P("seq", "ctx", "head", None),
        P("seq", "ctx", "head", None),
        P("head", None),
        P(),
        P("seq", "ctx", None),
        P("seq", "ctx", None),
        P(("seq", "ctx"), None, "head"),
        P(("seq", "ctx"), None, "head"),
        P(("seq", "ctx"), "head", None),
    )
    out_specs = P("seq", "ctx", "head")
    return jax.shard_map(body, mesh=mesh, in_specs=in_specs, out_specs=out_specs, check_vma=False)
```

```python
import math

import jax
import jax.numpy as jnp
from jax import lax
from jax.experimental import pallas as pl
from jax.experimental.pallas import tpu as pltpu
from jax.sharding import PartitionSpec as P

CAP = 16
MESH = pl.DeviceIdType.MESH
LOG2E = 1.4426950408889634
NEG = -3.0e38
NT = (((1,), (1,)), ((), ()))
GROUPS = 4
DEPTH = 768


def remote(src, dst, send, recv, where):
    return pltpu.make_async_remote_copy(
        src_ref=src, dst_ref=dst, send_sem=send, recv_sem=recv, device_id=where, device_id_type=MESH
    )


def layer_kernel(
    tok_hbm,
    qw_hbm,
    kt_hbm,
    vt_hbm,
    nk_hbm,
    nv_hbm,
    wo_hbm,
    gain_hbm,
    ids_hbm,
    weights_hbm,
    gate_hbm,
    up_hbm,
    down_hbm,
    out_ref,
    nk_ref,
    nv_ref,
    gain_ref,
    ids_ref,
    weights_ref,
    tok,
    qw,
    vt,
    own,
    gain,
    resid_s,
    qbuf,
    ke,
    ko,
    ve,
    vo,
    kn,
    vn,
    s_low,
    s_high,
    s_new,
    tops,
    level,
    p_new,
    half_acc,
    obuf,
    lbuf,
    rbuf_o,
    rlse,
    wo,
    pbuf,
    prec,
    raw,
    wide,
    wgu,
    wdn,
    select_s,
    factor_s,
    packed,
    xall,
    acc,
    hidden,
    sbuf,
    rbuf,
    final,
    back,
    in_sem,
    e_sem,
    q_send,
    q_recv,
    o_send,
    o_recv,
    l_send,
    l_recv,
    p_send,
    p_recv,
    w_sem,
    d_send,
    d_recv,
    g_send,
    g_recv,
    s_send,
    s_recv,
    b_send,
    b_recv,
):
    seqs, ctxs, heads = lax.axis_size("seq"), lax.axis_size("ctx"), lax.axis_size("head")
    s, c, h = lax.axis_index("seq"), lax.axis_index("ctx"), lax.axis_index("head")
    n, place, lane_of = ctxs, c, h
    experts = seqs * ctxs
    count, model = tok.shape
    width = own.shape[1]
    padded = wide.shape[1]
    block = ctxs * CAP
    f32, bf = jnp.float32, jnp.bfloat16
    ring = heads // 2
    col, y = lax.div(h, ring), lax.rem(h, ring)
    rows = qbuf.shape[1]
    half = ke.shape[0] // 2
    cached = ke.shape[1]
    pair = 2 * half

    def head_at(across, dy):
        return (col if across == 0 else 1 - col) * ring + lax.rem(y + dy + ring, ring)

    other, above, below = head_at(1, 0), head_at(0, 1), head_at(0, -1)
    edges = list(range(0, model, DEPTH)) + [model]
    spans = list(zip(edges[:-1], edges[1:]))
    tok_load = pltpu.make_async_copy(tok_hbm, tok, in_sem.at[0])
    qw_loads = [
        pltpu.make_async_copy(qw_hbm.at[low:high], qw.at[low:high], in_sem.at[4 + i])
        for i, (low, high) in enumerate(spans)
    ]
    kv_loads = [
        pltpu.make_async_copy(kt_hbm, ke.at[0:half], in_sem.at[1]),
        pltpu.make_async_copy(kt_hbm, ko.at[half:pair], in_sem.at[2]),
        pltpu.make_async_copy(vt_hbm, vt, in_sem.at[3]),
    ]
    small = [
        pltpu.make_async_copy(source, target, e_sem.at[i])
        for i, (source, target) in enumerate(
            (
                (nk_hbm, nk_ref),
                (nv_hbm, nv_ref),
                (gain_hbm, gain_ref),
                (ids_hbm, ids_ref),
                (weights_hbm, weights_ref),
            )
        )
    ]
    for load in [tok_load] + qw_loads + kv_loads + small:
        load.start()
    wo_copy = pltpu.make_async_copy(wo_hbm, wo, w_sem.at[3])
    loads = [
        pltpu.make_async_copy(source, raw.at[i], w_sem.at[i])
        for i, source in enumerate((gate_hbm, up_hbm, down_hbm))
    ]
    barrier = pltpu.get_barrier_semaphore()

    @pl.loop(1, experts)
    def _(step):
        there = {
            "seq": lax.rem(s + lax.div(step, ctxs), seqs),
            "ctx": lax.rem(c + lax.rem(step, ctxs), ctxs),
        }
        pl.semaphore_signal(barrier, inc=1, device_id=there, device_id_type=MESH)

    @pl.loop(1, heads)
    def _(step):
        there = {"head": lax.rem(h + step, heads)}
        pl.semaphore_signal(barrier, inc=1, device_id=there, device_id_type=MESH)

    ke[half:pair, :] = jnp.zeros((half, cached), bf)
    ko[0:half, :] = jnp.zeros((half, cached), bf)
    tok_load.wait()
    query = jnp.zeros((count, qw.shape[1]), f32)
    for (low_k, high_k), load in zip(spans, qw_loads):
        load.wait()
        query = query + jnp.dot(tok[:, low_k:high_k], qw[low_k:high_k, :], preferred_element_type=f32)
    query = (query.astype(bf).astype(f32) * (1.0 / math.sqrt(half))).astype(bf)
    for j in range(rows // count):
        qbuf[0, count * j : count * (j + 1), :] = query[:, pair * j : pair * (j + 1)]
    for load in kv_loads + small:
        load.wait()
    low_n = lax.broadcasted_iota(jnp.int32, (count, pair), 1) < half
    nk = nk_ref[...].astype(f32)
    nk = jnp.concatenate([nk, nk], axis=1)
    nv = nv_ref[...].astype(f32)
    nv = jnp.concatenate([nv, nv], axis=1)
    kn[0:count, :] = jnp.where(low_n, nk, 0.0).astype(bf)
    kn[count : 2 * count, :] = jnp.where(low_n, 0.0, nk).astype(bf)
    vn[0:count, 0:pair] = jnp.where(low_n, nv, 0.0).astype(bf)
    vn[count : 2 * count, 0:pair] = jnp.where(low_n, 0.0, nv).astype(bf)
    vn[0:count, pair : 2 * pair] = jnp.where(low_n, 1.0, 0.0).astype(bf)
    vn[count : 2 * count, pair : 2 * pair] = jnp.where(low_n, 0.0, 1.0).astype(bf)

    pl.semaphore_wait(barrier, experts - 1 + heads - 1)
    right = lax.rem(place + 1, n)
    left = lax.rem(place + n - 1, n)
    remote(qbuf.at[0], qbuf.at[1], q_send.at[1], q_recv.at[1], {"ctx": right}).start()
    remote(qbuf.at[0], qbuf.at[2], q_send.at[2], q_recv.at[2], {"ctx": left}).start()
    wo_copy.start()
    for load in loads:
        load.start()

    span = 256

    @pl.loop(0, cached // span)
    def _(i):
        at = pl.ds(pl.multiple_of(i * span, span), span)
        ones = jnp.where(lax.broadcasted_iota(jnp.int32, (span, pair), 1) < half, 1.0, 0.0)
        v = vt[:, at].astype(f32)
        blank = jnp.zeros_like(v)
        ve[at, 0:pair] = jnp.concatenate([v, blank], 0).T.astype(bf)
        vo[at, 0:pair] = jnp.concatenate([blank, v], 0).T.astype(bf)
        ve[at, pair : 2 * pair] = ones.astype(bf)
        vo[at, pair : 2 * pair] = (1.0 - ones).astype(bf)

    lane = lax.broadcasted_iota(jnp.int32, (rows, pair), 1)
    low = lane < half
    tokpos = lax.rem(lax.broadcasted_iota(jnp.int32, (rows, pair), 0), count)
    pos = lax.rem(lane, half)

    def source_of(k):
        return lax.rem(place + lax.div(k + 1, 2) * (1 - 2 * lax.rem(k, 2)) + n, n)

    def score_even(k, turn):
        q = qbuf[k]
        source = source_of(k)
        fresh = lax.dot_general(q, kn[...], NT, preferred_element_type=f32)
        ahead = jnp.where(place < source, count, jnp.where(place == source, 0, -count - 1))
        fresh = jnp.where(pos <= tokpos + ahead, fresh, NEG)
        s_new[turn] = fresh
        score = jnp.dot(q, ke[...], preferred_element_type=f32)
        s_low[...] = score
        peak = jnp.maximum(
            jnp.max(score, axis=1, keepdims=True),
            jnp.max(jnp.where(low, fresh, NEG), axis=1, keepdims=True),
        )
        tops[turn] = jnp.broadcast_to(peak, (rows, pair))

    score_even(0, 0)

    @pl.loop(0, n)
    def _(k):
        turn = lax.rem(k, 2)
        score = jnp.dot(qbuf[k], ko[...], preferred_element_type=f32)
        s_high[...] = score
        m_e = tops[turn]
        p_e = jnp.exp2((s_low[...] - m_e[:, 0:1]) * LOG2E).astype(bf)
        half_acc[...] = jnp.dot(p_e, ve[...], preferred_element_type=f32)
        m_o = jnp.maximum(
            jnp.max(score, axis=1, keepdims=True),
            jnp.max(jnp.where(low, NEG, s_new[turn]), axis=1, keepdims=True),
        )
        both = jnp.where(low, m_e, m_o)
        level[...] = both
        p_new[...] = jnp.exp2((s_new[turn] - both) * LOG2E).astype(bf)

        @pl.when(turn == 0)
        def _():
            for ahead, onward in ((1, right), (2, left)):
                at = k + ahead

                @pl.when(at < n)
                def _():
                    remote(qbuf.at[at], qbuf.at[at], q_send.at[at], q_recv.at[at], {"ctx": right}).wait_recv()

                    @pl.when(at + 2 < n)
                    def _():
                        remote(
                            qbuf.at[at], qbuf.at[at + 2], q_send.at[at + 2], q_recv.at[at + 2], {"ctx": onward}
                        ).start()

        score_even(jnp.minimum(k + 1, n - 1), 1 - turn)
        both = level[...]
        p_o = jnp.exp2((s_high[...] - both[:, half : half + 1]) * LOG2E).astype(bf)
        whole = (
            half_acc[...]
            + jnp.dot(p_o, vo[...], preferred_element_type=f32)
            + jnp.dot(p_new[...], vn[...], preferred_element_type=f32)
        )
        num = whole[:, 0:pair]
        tot = whole[:, pair : 2 * pair]
        obuf[k] = (num / tot).astype(bf)
        turned = (both + jnp.log(tot)).T
        for i in range(2):
            for j in range(2):
                lbuf[k, 2 * i + j : 2 * i + j + 1, :] = turned[i * half : i * half + 1, j * pair : (j + 1) * pair]

        @pl.when(k > 0)
        def _():
            there = {"ctx": source_of(k)}
            remote(obuf.at[k], rbuf_o.at[k], o_send.at[k], o_recv.at[k], there).start()
            remote(lbuf.at[k], rlse.at[k], l_send.at[k], l_recv.at[k], there).start()

    for i in range(heads):

        @pl.when(h == i)
        def _():
            own[...] = tok[:, i * width : (i + 1) * width].astype(f32)
            gain[...] = gain_ref[i * width : (i + 1) * width].reshape(1, width)

    ids = ids_ref[...]
    given = weights_ref[...]
    index = lax.broadcasted_iota(jnp.int32, (experts, count), 0)
    named = jnp.zeros((experts, count), f32)
    amount = jnp.zeros((experts, count), f32)
    for j in range(ids.shape[0]):
        hit = ids[j : j + 1, :] == index
        named = named + jnp.where(hit, 1.0, 0.0)
        amount = amount + jnp.where(hit, given[j : j + 1, :], 0.0)
    before = jnp.where(
        lax.broadcasted_iota(jnp.int32, (count, count), 0)
        < lax.broadcasted_iota(jnp.int32, (count, count), 1),
        1.0,
        0.0,
    ).astype(bf)
    rank = jnp.dot(named.astype(bf), before, preferred_element_type=f32)
    key = jnp.where(named > 0.5, rank, 128.0)
    spread = jnp.where(
        lax.div(lax.broadcasted_iota(jnp.int32, (experts * CAP, experts), 0), CAP)
        == lax.broadcasted_iota(jnp.int32, (experts * CAP, experts), 1),
        1.0,
        0.0,
    ).astype(bf)
    key = jnp.dot(spread, key.astype(bf), preferred_element_type=f32)
    slot = lax.rem(lax.broadcasted_iota(jnp.int32, (experts * CAP, count), 0), CAP).astype(f32)
    chosen = key == slot
    select_s[...] = jnp.where(chosen, 1.0, 0.0).astype(bf)

    def pieces(x):
        one = x.astype(bf)
        rest = x - one.astype(f32)
        two = rest.astype(bf)
        return one, two, (rest - two.astype(f32)).astype(bf)

    for i, piece in enumerate(pieces(amount)):
        on_slots = jnp.dot(spread, piece, preferred_element_type=f32)
        factor_s[i] = jnp.where(chosen, on_slots, 0.0).T.astype(bf)

    for load in loads:
        load.wait()
    tail = jnp.zeros((width, padded - width), bf)
    foot = jnp.zeros((padded - width, padded), bf)
    for i in range(heads):
        for j in range(2):
            wgu[i, j * padded : j * padded + width, :] = jnp.concatenate(
                [raw[j, :, i * width : (i + 1) * width], tail], axis=1
            )
            wgu[i, j * padded + width : (j + 1) * padded, :] = foot
        wdn[i, 0:width, :] = jnp.concatenate([raw[2, :, i * width : (i + 1) * width], tail], axis=1)
        wdn[i, width:padded, :] = foot
    wo_copy.wait()

    @pl.loop(1, n)
    def _(k):
        here = {"ctx": right}
        remote(obuf.at[k], rbuf_o.at[k], o_send.at[k], o_recv.at[k], here).wait_recv()
        remote(lbuf.at[k], rlse.at[k], l_send.at[k], l_recv.at[k], here).wait_recv()

    rbuf_o[0] = obuf[0]
    rlse[0] = lbuf[0]
    lse = [rlse[k] for k in range(n)]
    peak = lse[0]
    for k in range(1, n):
        peak = jnp.maximum(peak, lse[k])
    parts = [jnp.exp(x - peak) for x in lse]
    whole = parts[0]
    for k in range(1, n):
        whole = whole + parts[k]
    share = jnp.concatenate([x / whole for x in parts], axis=0)
    share = jnp.concatenate([share, share], axis=0).T
    upper = share.astype(bf).astype(f32)
    first = lax.broadcasted_iota(jnp.int32, share.shape, 1) < 4 * n
    split = jnp.where(first, upper, share - upper).astype(bf)
    spot = lax.broadcasted_iota(jnp.int32, (8 * n, pair * n), 1)
    line = lax.rem(lax.broadcasted_iota(jnp.int32, (8 * n, pair * n), 0), 4 * n)
    wanted = lax.div(spot, pair) * 4 + jnp.where(lax.rem(spot, pair) < half, 0, 2)
    halves = []
    for j in range(2):
        pick = jnp.where(line == wanted + j, 1.0, 0.0).astype(bf)
        factor = jnp.dot(split, pick, preferred_element_type=f32)
        total = jnp.zeros((pair, pair), f32)
        for k in range(n):
            total = total + factor[:, pair * k : pair * (k + 1)] * rbuf_o[k, j * pair : (j + 1) * pair, :].astype(f32)
        halves.append(total.astype(bf))
    attn = jnp.concatenate(halves, axis=0)
    flat = jnp.concatenate([attn[count * j : count * (j + 1), :] for j in range(rows // count)], axis=1)

    def peer_at(i):
        across = jnp.where(i < ring, 1 - col, col)
        dy = jnp.where(i < ring, 2 + i, i - ring + 1)
        return across * ring + lax.rem(y + dy, ring)

    @pl.loop(0, heads - 1)
    def _(i):
        there = peer_at(i)
        part = lax.dot_general(flat, wo[there], NT, preferred_element_type=f32)
        pbuf[i] = part.astype(bf)
        remote(pbuf.at[i], prec.at[i], p_send.at[i], p_recv.at[i], {"head": there}).start()

    mine = lax.dot_general(flat, wo[lane_of], NT, preferred_element_type=f32)
    total = own[...] + mine
    for i in range(heads - 1):
        there = peer_at(i)
        remote(pbuf.at[i], prec.at[i], p_send.at[i], p_recv.at[i], {"head": there}).wait_recv()
        total = total + prec[i].astype(f32)
    resid_s[...] = total

    resid = resid_s[...]
    wide[...] = jnp.zeros(wide.shape, f32)
    wide[:, 0:width] = resid * gain[...]
    power = jnp.sum(resid * resid, axis=1, keepdims=True)
    lane = lax.broadcasted_iota(jnp.int32, (count, padded), 1)
    row = wide[...]
    for i, piece in enumerate(pieces(power)):
        row = jnp.where(lane == width + i, piece.astype(f32), row)
    packed[...] = jnp.dot(select_s[...], row.astype(bf), preferred_element_type=f32).astype(bf)

    me = s * ctxs + c
    mine = pl.ds(pl.multiple_of(me * CAP, CAP), CAP)

    @pl.loop(1, experts)
    def _(step):
        s_to = lax.rem(s + seqs - lax.div(step, ctxs), seqs)
        c_to = lax.rem(c + lax.rem(step, ctxs), ctxs)
        at = pl.ds(pl.multiple_of((s_to * ctxs + c_to) * CAP, CAP), CAP)
        remote(
            packed.at[at], xall.at[0, mine], d_send.at[step], d_recv.at[step], {"seq": s_to, "ctx": c_to}
        ).start()

    xall[0, mine] = packed[mine]

    def rows_of(g):
        return pl.ds(pl.multiple_of(lax.rem(s + g, seqs) * block, block), block)

    def gather(kind, g, source, target):
        at = rows_of(g)
        return remote(
            xall.at[source, at],
            xall.at[kind, at],
            g_send.at[kind, g],
            g_recv.at[kind, g],
            {"head": target},
        )

    def stage_a(g):
        @pl.loop(1 if g == 0 else 0, ctxs)
        def _(dc):
            step = g * ctxs + dc
            at = pl.ds(0, CAP)
            remote(
                packed.at[at], xall.at[0, mine], d_send.at[step], d_recv.at[step], {"ctx": lax.rem(c + 1, ctxs)}
            ).wait_recv()

        gather(1, g, 0, other).start()
        gather(2, g, 0, above).start()
        gather(3, g, 0, below).start()

    def stage_b(g):
        gather(2, g, 0, above).wait_recv()
        gather(3, g, 0, below).wait_recv()
        if g % 2 == 0:
            gather(6, g, 2, above).start()
        else:
            gather(6, g, 3, below).start()
        gather(1, g, 0, other).wait_recv()
        gather(4, g, 1, above).start()
        gather(5, g, 1, below).start()

    def stage_c(g):
        gather(6, g, 2, above).wait_recv()
        gather(7, g, 6, other).start()

    slabs = [h, other, below, above, head_at(1, -1), head_at(1, 1), head_at(0, 2), head_at(1, 2)]

    def absorb(low, high):
        @pl.loop(low, high)
        def _(kind):
            where = slabs[low]
            for k in range(low + 1, high):
                where = jnp.where(kind == k, slabs[k], where)
            update = lax.dot_general(xall[kind], wgu[where], NT, preferred_element_type=f32)
            if low == 0:
                acc[...] = update
            else:
                acc[...] += update

    stage_a(0)
    stage_a(1)
    stage_b(0)
    stage_a(2)
    stage_b(1)
    stage_c(0)
    stage_a(3)
    stage_b(2)
    stage_c(1)
    absorb(0, 1)
    stage_b(3)
    stage_c(2)
    absorb(1, 4)
    stage_c(3)
    for g in range(GROUPS):
        gather(4, g, 1, above).wait_recv()
        gather(5, g, 1, below).wait_recv()
    absorb(4, 7)
    for g in range(GROUPS):
        gather(7, g, 6, other).wait_recv()
    absorb(7, 8)

    @pl.loop(0, GROUPS)
    def _(g):
        at = pl.ds(pl.multiple_of(g * block, block), block)
        tile = jnp.zeros((block, 128), f32)
        for k in range(heads):
            tile = tile + xall[k, at, padded - 128 : padded].astype(f32)
        spot = lax.broadcasted_iota(jnp.int32, (block, 128), 1) + (padded - 128)
        tile = jnp.where((spot >= width) & (spot < width + 3), tile, 0.0)
        power = jnp.sum(tile, axis=1, keepdims=True)
        scale = lax.rsqrt(power / (width * heads) + 1e-05)
        gate = acc[at, 0:padded] * scale
        up = acc[at, padded : 2 * padded] * scale
        hidden[at] = (gate * jax.nn.sigmoid(1.702 * gate) * (up + 1.0)).astype(bf)

    def part(g, target):
        return jnp.dot(hidden[rows_of(g)], wdn[target], preferred_element_type=f32)

    def scatter(kind, g, target):
        return remote(
            sbuf.at[kind, g], rbuf.at[kind, g], s_send.at[kind, g], s_recv.at[kind, g], {"head": target}
        )

    def got(kind, g):
        scatter(kind, g, other).wait_recv()
        return rbuf[kind, g].astype(f32)

    def send(kind, g, value, target):
        sbuf[kind, g] = value.astype(bf)
        scatter(kind, g, target).start()

    @pl.loop(0, GROUPS)
    def _(g):
        send(0, g, part(g, head_at(1, 2)), other)
        send(1, g, part(g, head_at(1, -1)), below)
        send(2, g, part(g, head_at(1, 1)), above)

    @pl.loop(0, GROUPS + 3)
    def _(t):
        @pl.when(t < GROUPS)
        def _():
            g = t
            value = part(g, head_at(0, 2)) + got(0, g)
            send(3, g, value, jnp.where(lax.rem(g, 2) == 0, above, below))
            value = part(g, other) + got(1, g) + got(2, g)
            send(4, g, value, other)

        @pl.when((t >= 1) & (t < GROUPS + 1))
        def _():
            g = t - 1
            even = lax.rem(g, 2) == 0

            @pl.when(even)
            def _():
                send(5, g, part(g, below), below)
                send(6, g, part(g, above) + got(3, g), above)

            @pl.when(jnp.logical_not(even))
            def _():
                send(6, g, part(g, above), above)
                send(5, g, part(g, below) + got(3, g), below)

        @pl.when(t >= 3)
        def _():
            g = t - 3
            value = part(g, h) + got(4, g) + got(5, g) + got(6, g)
            final[rows_of(g)] = value.astype(bf)
            s_to = lax.rem(s + g, seqs)

            @pl.loop(0, ctxs)
            def _(dc):
                @pl.when(g * ctxs + dc > 0)
                def _():
                    step = g * ctxs + dc
                    c_to = lax.rem(c + dc, ctxs)
                    at = pl.ds(pl.multiple_of((s_to * ctxs + c_to) * CAP, CAP), CAP)
                    remote(
                        final.at[at], back.at[mine], b_send.at[step], b_recv.at[step], {"seq": s_to, "ctx": c_to}
                    ).start()

    back[mine] = final[mine]

    def returned(step):
        at = pl.ds(0, CAP)
        return remote(
            final.at[at], back.at[mine], b_send.at[step], b_recv.at[step], {"ctx": lax.rem(c + 1, ctxs)}
        )

    @pl.loop(1, experts)
    def _(step):
        returned(step).wait_recv()

    moe = jnp.zeros((count, padded), f32)
    for i in range(3):
        moe = moe + jnp.dot(factor_s[i], back[...], preferred_element_type=f32)
    out_ref[...] = (resid_s[...] + moe[:, 0:width]).astype(bf)

    @pl.loop(1, experts)
    def _(step):
        at = pl.ds(0, CAP)
        remote(
            packed.at[at], xall.at[0, mine], d_send.at[step], d_recv.at[step], {"ctx": lax.rem(c + 1, ctxs)}
        ).wait_send()
        returned(step).wait_send()

    for g in range(GROUPS):
        for kind in range(1, heads):
            gather(kind, g, 0, other).wait_send()
        for kind in range(heads - 1):
            scatter(kind, g, other).wait_send()

    @pl.loop(1, n)
    def _(k):
        here = {"ctx": right}
        remote(qbuf.at[k], qbuf.at[k], q_send.at[k], q_recv.at[k], here).wait_send()
        remote(obuf.at[k], rbuf_o.at[k], o_send.at[k], o_recv.at[k], here).wait_send()
        remote(lbuf.at[k], rlse.at[k], l_send.at[k], l_recv.at[k], here).wait_send()

    @pl.loop(0, heads - 1)
    def _(c):
        there = lax.rem(lane_of + 1 + c, heads)
        remote(pbuf.at[c], prec.at[c], p_send.at[c], p_recv.at[c], {"head": there}).wait_send()


def layer(tokens, qw, kt, vt, nk, nv, wo, gain, ids, weights, gate, up, down):
    seqs, ctxs, heads = lax.axis_size("seq"), lax.axis_size("ctx"), lax.axis_size("head")
    experts = seqs * ctxs
    slots = experts * CAP
    count, model = tokens.shape
    width = model // heads
    half, cached = kt.shape
    pair = 2 * half
    rows = qw.shape[1] // pair * count
    hidden = gate.shape[0]
    padded = -(-(width + 3) // 128) * 128
    block = ctxs * CAP
    bf, f32 = jnp.bfloat16, jnp.float32
    vm = pl.BlockSpec(memory_space=pltpu.VMEM)
    hbm = pl.BlockSpec(memory_space=pl.ANY)
    dma = pltpu.SemaphoreType.DMA
    spans = -(-model // DEPTH)
    return pl.pallas_call(
        layer_kernel,
        out_shape=jax.ShapeDtypeStruct((count, width), bf),
        in_specs=[hbm] * 13,
        out_specs=vm,
        scratch_shapes=[
            pltpu.VMEM(nk.shape, bf),
            pltpu.VMEM(nv.shape, bf),
            pltpu.VMEM(gain.shape, f32),
            pltpu.VMEM(ids.shape, jnp.int32),
            pltpu.VMEM(weights.shape, f32),
            pltpu.VMEM((count, model), bf),
            pltpu.VMEM(qw.shape, bf),
            pltpu.VMEM(vt.shape, bf),
            pltpu.VMEM((count, width), f32),
            pltpu.VMEM((1, width), f32),
            pltpu.VMEM((count, width), f32),
            pltpu.VMEM((ctxs, rows, pair), bf),
            pltpu.VMEM((pair, cached), bf),
            pltpu.VMEM((pair, cached), bf),
            pltpu.VMEM((cached, 2 * pair), bf),
            pltpu.VMEM((cached, 2 * pair), bf),
            pltpu.VMEM((2 * count, pair), bf),
            pltpu.VMEM((2 * count, 2 * pair), bf),
            pltpu.VMEM((rows, cached), f32),
            pltpu.VMEM((rows, cached), f32),
            pltpu.VMEM((2, rows, pair), f32),
            pltpu.VMEM((2, rows, pair), f32),
            pltpu.VMEM((rows, pair), f32),
            pltpu.VMEM((rows, pair), bf),
            pltpu.VMEM((rows, 2 * pair), f32),
            pltpu.VMEM((ctxs, rows, pair), bf),
            pltpu.VMEM((ctxs, 4, pair), f32),
            pltpu.VMEM((ctxs, rows, pair), bf),
            pltpu.VMEM((ctxs, 4, pair), f32),
            pltpu.VMEM(wo.shape, bf),
            pltpu.VMEM((heads - 1, count, width), bf),
            pltpu.VMEM((heads - 1, count, width), bf),
            pltpu.VMEM((3, hidden, model), bf),
            pltpu.VMEM((count, padded), f32),
            pltpu.VMEM((heads, 2 * padded, padded), bf),
            pltpu.VMEM((heads, padded, padded), bf),
            pltpu.VMEM((slots, count), bf),
            pltpu.VMEM((3, count, slots), bf),
            pltpu.VMEM((slots, padded), bf),
            pltpu.VMEM((heads, slots, padded), bf),
            pltpu.VMEM((slots, 2 * padded), f32),
            pltpu.VMEM((slots, padded), bf),
            pltpu.VMEM((heads - 1, GROUPS, block, padded), bf),
            pltpu.VMEM((heads - 1, GROUPS, block, padded), bf),
            pltpu.VMEM((slots, padded), bf),
            pltpu.VMEM((slots, padded), bf),
            dma((4 + spans,)),
            dma((5,)),
            dma((ctxs,)),
            dma((ctxs,)),
            dma((ctxs,)),
            dma((ctxs,)),
            dma((ctxs,)),
            dma((ctxs,)),
            dma((heads - 1,)),
            dma((heads - 1,)),
            dma((4,)),
            dma((experts,)),
            dma((experts,)),
            dma((heads, GROUPS)),
            dma((heads, GROUPS)),
            dma((heads - 1, GROUPS)),
            dma((heads - 1, GROUPS)),
            dma((experts,)),
            dma((experts,)),
        ],
        compiler_params=pltpu.CompilerParams(
            collective_id=0, has_side_effects=True, vmem_limit_bytes=56 * 1024 * 1024
        ),
    )(tokens, qw, kt, vt, nk, nv, wo, gain, ids, weights, gate, up, down)


def body(
    stream,
    query_weight,
    cache_keys,
    cache_values,
    new_keys,
    new_values,
    out_weight,
    norm_gain,
    expert_ids,
    expert_weights,
    gate_weight,
    up_weight,
    down_weight,
):
    heads = lax.axis_size("head")
    taken, model = out_weight.shape
    mixed = layer(
        stream[0],
        query_weight,
        cache_keys[0, :, 0, :].T,
        cache_values[0, :, 0, :].T,
        new_keys[0, :, 0, :],
        new_values[0, :, 0, :],
        out_weight.T.reshape(heads, model // heads, taken),
        norm_gain,
        expert_ids[0].T,
        expert_weights[0].T,
        gate_weight[0].T,
        up_weight[0].T,
        down_weight[0],
    )
    return mixed[None]


def solution(mesh):
    in_specs = (
        P("seq", "ctx", None),
        P(None, "head"),
        P("seq", "ctx", "head", None),
        P("seq", "ctx", "head", None),
        P("seq", "ctx", "head", None),
        P("seq", "ctx", "head", None),
        P("head", None),
        P(),
        P("seq", "ctx", None),
        P("seq", "ctx", None),
        P(("seq", "ctx"), None, "head"),
        P(("seq", "ctx"), None, "head"),
        P(("seq", "ctx"), "head", None),
    )
    out_specs = P("seq", "ctx", "head")
    return jax.shard_map(body, mesh=mesh, in_specs=in_specs, out_specs=out_specs, check_vma=False)
```

```python
import math

import jax
import jax.numpy as jnp
from jax import lax
from jax.experimental import pallas as pl
from jax.experimental.pallas import tpu as pltpu
from jax.sharding import PartitionSpec as P

CAP = 16
MESH = pl.DeviceIdType.MESH
LOG2E = 1.4426950408889634
NEG = -3.0e38
NT = (((1,), (1,)), ((), ()))
GROUPS = 4
DEPTH = 768


def remote(src, dst, send, recv, where):
    return pltpu.make_async_remote_copy(
        src_ref=src, dst_ref=dst, send_sem=send, recv_sem=recv, device_id=where, device_id_type=MESH
    )


def layer_kernel(
    tok_hbm,
    qw_hbm,
    kt_hbm,
    vt_hbm,
    nk_hbm,
    nv_hbm,
    wo_hbm,
    gain_hbm,
    ids_hbm,
    weights_hbm,
    gate_hbm,
    up_hbm,
    down_hbm,
    out_ref,
    nk_ref,
    nv_ref,
    gain_ref,
    ids_ref,
    weights_ref,
    tok,
    qw,
    vt,
    own,
    gain,
    resid_s,
    qbuf,
    ke,
    ko,
    ve,
    vo,
    kn,
    vn,
    s_low,
    s_high,
    s_new,
    tops,
    level,
    p_new,
    half_acc,
    obuf,
    lbuf,
    rbuf_o,
    rlse,
    wo,
    pbuf,
    prec,
    raw,
    wide,
    wgu,
    wdn,
    select_s,
    factor_s,
    packed,
    xall,
    acc,
    hidden,
    sbuf,
    rbuf,
    final,
    back,
    in_sem,
    e_sem,
    q_send,
    q_recv,
    o_send,
    o_recv,
    l_send,
    l_recv,
    p_send,
    p_recv,
    w_sem,
    d_send,
    d_recv,
    g_send,
    g_recv,
    s_send,
    s_recv,
    b_send,
    b_recv,
):
    seqs, ctxs, heads = lax.axis_size("seq"), lax.axis_size("ctx"), lax.axis_size("head")
    s, c, h = lax.axis_index("seq"), lax.axis_index("ctx"), lax.axis_index("head")
    n, place, lane_of = ctxs, c, h
    experts = seqs * ctxs
    count, model = tok.shape
    width = own.shape[1]
    padded = wide.shape[1]
    block = ctxs * CAP
    f32, bf = jnp.float32, jnp.bfloat16
    ring = heads // 2
    col, y = lax.div(h, ring), lax.rem(h, ring)
    rows = qbuf.shape[1]
    half = ke.shape[0] // 2
    cached = ke.shape[1]
    pair = 2 * half

    def head_at(across, dy):
        return (col if across == 0 else 1 - col) * ring + lax.rem(y + dy + ring, ring)

    other, above, below = head_at(1, 0), head_at(0, 1), head_at(0, -1)
    edges = list(range(0, model, DEPTH)) + [model]
    spans = list(zip(edges[:-1], edges[1:]))
    tok_load = pltpu.make_async_copy(tok_hbm, tok, in_sem.at[0])
    qw_loads = [
        pltpu.make_async_copy(qw_hbm.at[low:high], qw.at[low:high], in_sem.at[4 + i])
        for i, (low, high) in enumerate(spans)
    ]
    kv_loads = [
        pltpu.make_async_copy(kt_hbm, ke.at[0:half], in_sem.at[1]),
        pltpu.make_async_copy(kt_hbm, ko.at[half:pair], in_sem.at[2]),
        pltpu.make_async_copy(vt_hbm, vt, in_sem.at[3]),
    ]
    small = [
        pltpu.make_async_copy(source, target, e_sem.at[i])
        for i, (source, target) in enumerate(
            (
                (nk_hbm, nk_ref),
                (nv_hbm, nv_ref),
                (gain_hbm, gain_ref),
                (ids_hbm, ids_ref),
                (weights_hbm, weights_ref),
            )
        )
    ]
    for load in [tok_load] + qw_loads + kv_loads + small:
        load.start()
    wo_copy = pltpu.make_async_copy(wo_hbm, wo, w_sem.at[3])
    loads = [
        pltpu.make_async_copy(source, raw.at[i], w_sem.at[i])
        for i, source in enumerate((gate_hbm, up_hbm, down_hbm))
    ]
    barrier = pltpu.get_barrier_semaphore()

    @pl.loop(1, experts)
    def _(step):
        there = {
            "seq": lax.rem(s + lax.div(step, ctxs), seqs),
            "ctx": lax.rem(c + lax.rem(step, ctxs), ctxs),
        }
        pl.semaphore_signal(barrier, inc=1, device_id=there, device_id_type=MESH)

    @pl.loop(1, heads)
    def _(step):
        there = {"head": lax.rem(h + step, heads)}
        pl.semaphore_signal(barrier, inc=1, device_id=there, device_id_type=MESH)

    ke[half:pair, :] = jnp.zeros((half, cached), bf)
    ko[0:half, :] = jnp.zeros((half, cached), bf)
    tok_load.wait()
    query = jnp.zeros((count, qw.shape[1]), f32)
    for (low_k, high_k), load in zip(spans, qw_loads):
        load.wait()
        query = query + jnp.dot(tok[:, low_k:high_k], qw[low_k:high_k, :], preferred_element_type=f32)
    query = (query.astype(bf).astype(f32) * (1.0 / math.sqrt(half))).astype(bf)
    for j in range(rows // count):
        qbuf[0, count * j : count * (j + 1), :] = query[:, pair * j : pair * (j + 1)]
    for load in kv_loads + small:
        load.wait()
    low_n = lax.broadcasted_iota(jnp.int32, (count, pair), 1) < half
    nk = nk_ref[...].astype(f32)
    nk = jnp.concatenate([nk, nk], axis=1)
    nv = nv_ref[...].astype(f32)
    nv = jnp.concatenate([nv, nv], axis=1)
    kn[0:count, :] = jnp.where(low_n, nk, 0.0).astype(bf)
    kn[count : 2 * count, :] = jnp.where(low_n, 0.0, nk).astype(bf)
    vn[0:count, 0:pair] = jnp.where(low_n, nv, 0.0).astype(bf)
    vn[count : 2 * count, 0:pair] = jnp.where(low_n, 0.0, nv).astype(bf)
    vn[0:count, pair : 2 * pair] = jnp.where(low_n, 1.0, 0.0).astype(bf)
    vn[count : 2 * count, pair : 2 * pair] = jnp.where(low_n, 0.0, 1.0).astype(bf)

    pl.semaphore_wait(barrier, experts - 1 + heads - 1)
    right = lax.rem(place + 1, n)
    left = lax.rem(place + n - 1, n)
    remote(qbuf.at[0], qbuf.at[1], q_send.at[1], q_recv.at[1], {"ctx": right}).start()
    remote(qbuf.at[0], qbuf.at[2], q_send.at[2], q_recv.at[2], {"ctx": left}).start()
    wo_copy.start()
    for load in loads:
        load.start()

    span = 256

    @pl.loop(0, cached // span)
    def _(i):
        at = pl.ds(pl.multiple_of(i * span, span), span)
        ones = jnp.where(lax.broadcasted_iota(jnp.int32, (span, pair), 1) < half, 1.0, 0.0)
        v = vt[:, at].astype(f32)
        blank = jnp.zeros_like(v)
        ve[at, 0:pair] = jnp.concatenate([v, blank], 0).T.astype(bf)
        vo[at, 0:pair] = jnp.concatenate([blank, v], 0).T.astype(bf)
        ve[at, pair : 2 * pair] = ones.astype(bf)
        vo[at, pair : 2 * pair] = (1.0 - ones).astype(bf)

    lane = lax.broadcasted_iota(jnp.int32, (rows, pair), 1)
    low = lane < half
    tokpos = lax.rem(lax.broadcasted_iota(jnp.int32, (rows, pair), 0), count)
    pos = lax.rem(lane, half)

    def source_of(k):
        return lax.rem(place + lax.div(k + 1, 2) * (1 - 2 * lax.rem(k, 2)) + n, n)

    def score_even(k, turn):
        q = qbuf[k]
        source = source_of(k)
        fresh = lax.dot_general(q, kn[...], NT, preferred_element_type=f32)
        ahead = jnp.where(place < source, count, jnp.where(place == source, 0, -count - 1))
        fresh = jnp.where(pos <= tokpos + ahead, fresh, NEG)
        s_new[turn] = fresh
        score = jnp.dot(q, ke[...], preferred_element_type=f32)
        s_low[...] = score
        peak = jnp.maximum(
            jnp.max(score, axis=1, keepdims=True),
            jnp.max(jnp.where(low, fresh, NEG), axis=1, keepdims=True),
        )
        tops[turn] = jnp.broadcast_to(peak, (rows, pair))

    score_even(0, 0)

    @pl.loop(0, n)
    def _(k):
        turn = lax.rem(k, 2)
        score = jnp.dot(qbuf[k], ko[...], preferred_element_type=f32)
        s_high[...] = score
        m_e = tops[turn]
        p_e = jnp.exp2((s_low[...] - m_e[:, 0:1]) * LOG2E).astype(bf)
        half_acc[...] = jnp.dot(p_e, ve[...], preferred_element_type=f32)
        m_o = jnp.maximum(
            jnp.max(score, axis=1, keepdims=True),
            jnp.max(jnp.where(low, NEG, s_new[turn]), axis=1, keepdims=True),
        )
        both = jnp.where(low, m_e, m_o)
        level[...] = both
        p_new[...] = jnp.exp2((s_new[turn] - both) * LOG2E).astype(bf)

        @pl.when(turn == 0)
        def _():
            for ahead, onward in ((1, right), (2, left)):
                at = k + ahead

                @pl.when(at < n)
                def _():
                    remote(qbuf.at[at], qbuf.at[at], q_send.at[at], q_recv.at[at], {"ctx": right}).wait_recv()

                    @pl.when(at + 2 < n)
                    def _():
                        remote(
                            qbuf.at[at], qbuf.at[at + 2], q_send.at[at + 2], q_recv.at[at + 2], {"ctx": onward}
                        ).start()

        score_even(jnp.minimum(k + 1, n - 1), 1 - turn)
        both = level[...]
        p_o = jnp.exp2((s_high[...] - both[:, half : half + 1]) * LOG2E).astype(bf)
        whole = (
            half_acc[...]
            + jnp.dot(p_o, vo[...], preferred_element_type=f32)
            + jnp.dot(p_new[...], vn[...], preferred_element_type=f32)
        )
        num = whole[:, 0:pair]
        tot = whole[:, pair : 2 * pair]
        obuf[k] = (num / tot).astype(bf)
        turned = (both + jnp.log(tot)).T
        for i in range(2):
            for j in range(2):
                lbuf[k, 2 * i + j : 2 * i + j + 1, :] = turned[i * half : i * half + 1, j * pair : (j + 1) * pair]

        @pl.when(k > 0)
        def _():
            there = {"ctx": source_of(k)}
            remote(obuf.at[k], rbuf_o.at[k], o_send.at[k], o_recv.at[k], there).start()
            remote(lbuf.at[k], rlse.at[k], l_send.at[k], l_recv.at[k], there).start()

    for i in range(heads):

        @pl.when(h == i)
        def _():
            own[...] = tok[:, i * width : (i + 1) * width].astype(f32)
            gain[...] = gain_ref[i * width : (i + 1) * width].reshape(1, width)

    ids = ids_ref[...]
    given = weights_ref[...]
    index = lax.broadcasted_iota(jnp.int32, (experts, count), 0)
    named = jnp.zeros((experts, count), f32)
    amount = jnp.zeros((experts, count), f32)
    for j in range(ids.shape[0]):
        hit = ids[j : j + 1, :] == index
        named = named + jnp.where(hit, 1.0, 0.0)
        amount = amount + jnp.where(hit, given[j : j + 1, :], 0.0)
    before = jnp.where(
        lax.broadcasted_iota(jnp.int32, (count, count), 0)
        < lax.broadcasted_iota(jnp.int32, (count, count), 1),
        1.0,
        0.0,
    ).astype(bf)
    rank = jnp.dot(named.astype(bf), before, preferred_element_type=f32)
    key = jnp.where(named > 0.5, rank, 128.0)
    spread = jnp.where(
        lax.div(lax.broadcasted_iota(jnp.int32, (experts * CAP, experts), 0), CAP)
        == lax.broadcasted_iota(jnp.int32, (experts * CAP, experts), 1),
        1.0,
        0.0,
    ).astype(bf)
    key = jnp.dot(spread, key.astype(bf), preferred_element_type=f32)
    slot = lax.rem(lax.broadcasted_iota(jnp.int32, (experts * CAP, count), 0), CAP).astype(f32)
    chosen = key == slot
    select_s[...] = jnp.where(chosen, 1.0, 0.0).astype(bf)

    def pieces(x):
        one = x.astype(bf)
        rest = x - one.astype(f32)
        two = rest.astype(bf)
        return one, two, (rest - two.astype(f32)).astype(bf)

    for i, piece in enumerate(pieces(amount)):
        on_slots = jnp.dot(spread, piece, preferred_element_type=f32)
        factor_s[i] = jnp.where(chosen, on_slots, 0.0).T.astype(bf)

    for load in loads:
        load.wait()
    tail = jnp.zeros((width, padded - width), bf)
    foot = jnp.zeros((padded - width, padded), bf)
    for i in range(heads):
        for j in range(2):
            wgu[i, j * padded : j * padded + width, :] = jnp.concatenate(
                [raw[j, :, i * width : (i + 1) * width], tail], axis=1
            )
            wgu[i, j * padded + width : (j + 1) * padded, :] = foot
        wdn[i, 0:width, :] = jnp.concatenate([raw[2, :, i * width : (i + 1) * width], tail], axis=1)
        wdn[i, width:padded, :] = foot
    wo_copy.wait()

    @pl.loop(1, n)
    def _(k):
        here = {"ctx": right}
        remote(obuf.at[k], rbuf_o.at[k], o_send.at[k], o_recv.at[k], here).wait_recv()
        remote(lbuf.at[k], rlse.at[k], l_send.at[k], l_recv.at[k], here).wait_recv()

    rbuf_o[0] = obuf[0]
    rlse[0] = lbuf[0]
    lse = [rlse[k] for k in range(n)]
    peak = lse[0]
    for k in range(1, n):
        peak = jnp.maximum(peak, lse[k])
    parts = [jnp.exp(x - peak) for x in lse]
    whole = parts[0]
    for k in range(1, n):
        whole = whole + parts[k]
    share = jnp.concatenate([x / whole for x in parts], axis=0)
    share = jnp.concatenate([share, share], axis=0).T
    upper = share.astype(bf).astype(f32)
    first = lax.broadcasted_iota(jnp.int32, share.shape, 1) < 4 * n
    split = jnp.where(first, upper, share - upper).astype(bf)
    spot = lax.broadcasted_iota(jnp.int32, (8 * n, pair * n), 1)
    line = lax.rem(lax.broadcasted_iota(jnp.int32, (8 * n, pair * n), 0), 4 * n)
    wanted = lax.div(spot, pair) * 4 + jnp.where(lax.rem(spot, pair) < half, 0, 2)
    halves = []
    for j in range(2):
        pick = jnp.where(line == wanted + j, 1.0, 0.0).astype(bf)
        factor = jnp.dot(split, pick, preferred_element_type=f32)
        total = jnp.zeros((pair, pair), f32)
        for k in range(n):
            total = total + factor[:, pair * k : pair * (k + 1)] * rbuf_o[k, j * pair : (j + 1) * pair, :].astype(f32)
        halves.append(total.astype(bf))
    attn = jnp.concatenate(halves, axis=0)
    flat = jnp.concatenate([attn[count * j : count * (j + 1), :] for j in range(rows // count)], axis=1)

    def peer_at(i):
        across = jnp.where(i < ring, 1 - col, col)
        dy = jnp.where(i < ring, 2 + i, i - ring + 1)
        return across * ring + lax.rem(y + dy, ring)

    @pl.loop(0, heads - 1)
    def _(i):
        there = peer_at(i)
        part = lax.dot_general(flat, wo[there], NT, preferred_element_type=f32)
        pbuf[i] = part.astype(bf)
        remote(pbuf.at[i], prec.at[i], p_send.at[i], p_recv.at[i], {"head": there}).start()

    mine = lax.dot_general(flat, wo[lane_of], NT, preferred_element_type=f32)
    total = own[...] + mine
    for i in range(heads - 1):
        there = peer_at(i)
        remote(pbuf.at[i], prec.at[i], p_send.at[i], p_recv.at[i], {"head": there}).wait_recv()
        total = total + prec[i].astype(f32)
    resid_s[...] = total

    resid = resid_s[...]
    wide[...] = jnp.zeros(wide.shape, f32)
    wide[:, 0:width] = resid * gain[...]
    power = jnp.sum(resid * resid, axis=1, keepdims=True)
    lane = lax.broadcasted_iota(jnp.int32, (count, padded), 1)
    row = wide[...]
    for i, piece in enumerate(pieces(power)):
        row = jnp.where(lane == width + i, piece.astype(f32), row)
    packed[...] = jnp.dot(select_s[...], row.astype(bf), preferred_element_type=f32).astype(bf)

    me = s * ctxs + c
    mine = pl.ds(pl.multiple_of(me * CAP, CAP), CAP)

    @pl.loop(0, experts)
    def _(turn):
        step = turn - lax.rem(turn, ctxs) + lax.rem(turn + ctxs // 2, ctxs)
        s_to = lax.rem(s + seqs - lax.div(step, ctxs), seqs)
        c_to = lax.rem(c + lax.rem(step, ctxs), ctxs)
        at = pl.ds(pl.multiple_of((s_to * ctxs + c_to) * CAP, CAP), CAP)

        @pl.when(step > 0)
        def _():
            remote(
                packed.at[at], xall.at[0, mine], d_send.at[step], d_recv.at[step], {"seq": s_to, "ctx": c_to}
            ).start()

    xall[0, mine] = packed[mine]

    def rows_of(g):
        return pl.ds(pl.multiple_of(lax.rem(s + g, seqs) * block, block), block)

    def gather(kind, g, source, target):
        at = rows_of(g)
        return remote(
            xall.at[source, at],
            xall.at[kind, at],
            g_send.at[kind, g],
            g_recv.at[kind, g],
            {"head": target},
        )

    def stage_a(g):
        @pl.loop(1 if g == 0 else 0, ctxs)
        def _(dc):
            step = g * ctxs + dc
            at = pl.ds(0, CAP)
            remote(
                packed.at[at], xall.at[0, mine], d_send.at[step], d_recv.at[step], {"ctx": lax.rem(c + 1, ctxs)}
            ).wait_recv()

        gather(1, g, 0, other).start()
        gather(2, g, 0, above).start()
        gather(3, g, 0, below).start()

    def stage_b(g):
        gather(2, g, 0, above).wait_recv()
        gather(3, g, 0, below).wait_recv()
        if g % 2 == 0:
            gather(6, g, 2, above).start()
        else:
            gather(6, g, 3, below).start()
        gather(1, g, 0, other).wait_recv()
        gather(4, g, 1, above).start()
        gather(5, g, 1, below).start()

    def stage_c(g):
        gather(6, g, 2, above).wait_recv()
        gather(7, g, 6, other).start()

    slabs = [h, other, below, above, head_at(1, -1), head_at(1, 1), head_at(0, 2), head_at(1, 2)]

    def absorb(low, high):
        @pl.loop(low, high)
        def _(kind):
            where = slabs[low]
            for k in range(low + 1, high):
                where = jnp.where(kind == k, slabs[k], where)
            update = lax.dot_general(xall[kind], wgu[where], NT, preferred_element_type=f32)
            if low == 0:
                acc[...] = update
            else:
                acc[...] += update

    stage_a(0)
    stage_a(1)
    stage_b(0)
    stage_a(2)
    stage_b(1)
    stage_c(0)
    stage_a(3)
    stage_b(2)
    stage_c(1)
    absorb(0, 1)
    stage_b(3)
    stage_c(2)
    absorb(1, 4)
    stage_c(3)
    for g in range(GROUPS):
        gather(4, g, 1, above).wait_recv()
        gather(5, g, 1, below).wait_recv()
    absorb(4, 7)
    for g in range(GROUPS):
        gather(7, g, 6, other).wait_recv()
    absorb(7, 8)

    def rows_back(g):
        return rows_of(GROUPS - 1 - g)

    def activate(g):
        at = rows_back(g)
        tile = jnp.zeros((block, 128), f32)
        for k in range(heads):
            tile = tile + xall[k, at, padded - 128 : padded].astype(f32)
        spot = lax.broadcasted_iota(jnp.int32, (block, 128), 1) + (padded - 128)
        tile = jnp.where((spot >= width) & (spot < width + 3), tile, 0.0)
        power = jnp.sum(tile, axis=1, keepdims=True)
        scale = lax.rsqrt(power / (width * heads) + 1e-05)
        gate = acc[at, 0:padded] * scale
        up = acc[at, padded : 2 * padded] * scale
        hidden[at] = (gate * jax.nn.sigmoid(1.702 * gate) * (up + 1.0)).astype(bf)

    def part(g, target):
        return jnp.dot(hidden[rows_back(g)], wdn[target], preferred_element_type=f32)

    def scatter(kind, g, target):
        return remote(
            sbuf.at[kind, g], rbuf.at[kind, g], s_send.at[kind, g], s_recv.at[kind, g], {"head": target}
        )

    def got(kind, g):
        scatter(kind, g, other).wait_recv()
        return rbuf[kind, g].astype(f32)

    def send(kind, g, value, target):
        sbuf[kind, g] = value.astype(bf)
        scatter(kind, g, target).start()

    @pl.loop(0, GROUPS)
    def _(g):
        activate(g)
        send(0, g, part(g, head_at(1, 2)), other)
        send(1, g, part(g, head_at(1, -1)), below)
        send(2, g, part(g, head_at(1, 1)), above)

    @pl.loop(0, GROUPS + 3)
    def _(t):
        @pl.when(t < GROUPS)
        def _():
            g = t
            value = part(g, head_at(0, 2)) + got(0, g)
            send(3, g, value, jnp.where(lax.rem(g, 2) == 0, above, below))
            value = part(g, other) + got(1, g) + got(2, g)
            send(4, g, value, other)

        @pl.when((t >= 1) & (t < GROUPS + 1))
        def _():
            g = t - 1
            even = lax.rem(g, 2) == 0

            @pl.when(even)
            def _():
                send(5, g, part(g, below), below)
                send(6, g, part(g, above) + got(3, g), above)

            @pl.when(jnp.logical_not(even))
            def _():
                send(6, g, part(g, above), above)
                send(5, g, part(g, below) + got(3, g), below)

        @pl.when(t >= 3)
        def _():
            g = t - 3
            value = part(g, h) + got(4, g) + got(5, g) + got(6, g)
            final[rows_back(g)] = value.astype(bf)
            away = GROUPS - 1 - g
            s_to = lax.rem(s + away, seqs)

            @pl.loop(0, ctxs)
            def _(order):
                dc = lax.rem(order + ctxs // 2, ctxs)

                @pl.when(away * ctxs + dc > 0)
                def _():
                    step = away * ctxs + dc
                    c_to = lax.rem(c + dc, ctxs)
                    at = pl.ds(pl.multiple_of((s_to * ctxs + c_to) * CAP, CAP), CAP)
                    remote(
                        final.at[at], back.at[mine], b_send.at[step], b_recv.at[step], {"seq": s_to, "ctx": c_to}
                    ).start()

    back[mine] = final[mine]

    def returned(step):
        at = pl.ds(0, CAP)
        return remote(
            final.at[at], back.at[mine], b_send.at[step], b_recv.at[step], {"ctx": lax.rem(c + 1, ctxs)}
        )

    @pl.loop(1, experts)
    def _(step):
        returned(step).wait_recv()

    moe = jnp.zeros((count, padded), f32)
    for i in range(3):
        moe = moe + jnp.dot(factor_s[i], back[...], preferred_element_type=f32)
    out_ref[...] = (resid_s[...] + moe[:, 0:width]).astype(bf)

    @pl.loop(1, experts)
    def _(step):
        at = pl.ds(0, CAP)
        remote(
            packed.at[at], xall.at[0, mine], d_send.at[step], d_recv.at[step], {"ctx": lax.rem(c + 1, ctxs)}
        ).wait_send()
        returned(step).wait_send()

    for g in range(GROUPS):
        for kind in range(1, heads):
            gather(kind, g, 0, other).wait_send()
        for kind in range(heads - 1):
            scatter(kind, g, other).wait_send()

    @pl.loop(1, n)
    def _(k):
        here = {"ctx": right}
        remote(qbuf.at[k], qbuf.at[k], q_send.at[k], q_recv.at[k], here).wait_send()
        remote(obuf.at[k], rbuf_o.at[k], o_send.at[k], o_recv.at[k], here).wait_send()
        remote(lbuf.at[k], rlse.at[k], l_send.at[k], l_recv.at[k], here).wait_send()

    @pl.loop(0, heads - 1)
    def _(c):
        there = lax.rem(lane_of + 1 + c, heads)
        remote(pbuf.at[c], prec.at[c], p_send.at[c], p_recv.at[c], {"head": there}).wait_send()


def layer(tokens, qw, kt, vt, nk, nv, wo, gain, ids, weights, gate, up, down):
    seqs, ctxs, heads = lax.axis_size("seq"), lax.axis_size("ctx"), lax.axis_size("head")
    experts = seqs * ctxs
    slots = experts * CAP
    count, model = tokens.shape
    width = model // heads
    half, cached = kt.shape
    pair = 2 * half
    rows = qw.shape[1] // pair * count
    hidden = gate.shape[0]
    padded = -(-(width + 3) // 128) * 128
    block = ctxs * CAP
    bf, f32 = jnp.bfloat16, jnp.float32
    vm = pl.BlockSpec(memory_space=pltpu.VMEM)
    hbm = pl.BlockSpec(memory_space=pl.ANY)
    dma = pltpu.SemaphoreType.DMA
    spans = -(-model // DEPTH)
    return pl.pallas_call(
        layer_kernel,
        out_shape=jax.ShapeDtypeStruct((count, width), bf),
        in_specs=[hbm] * 13,
        out_specs=vm,
        scratch_shapes=[
            pltpu.VMEM(nk.shape, bf),
            pltpu.VMEM(nv.shape, bf),
            pltpu.VMEM(gain.shape, f32),
            pltpu.VMEM(ids.shape, jnp.int32),
            pltpu.VMEM(weights.shape, f32),
            pltpu.VMEM((count, model), bf),
            pltpu.VMEM(qw.shape, bf),
            pltpu.VMEM(vt.shape, bf),
            pltpu.VMEM((count, width), f32),
            pltpu.VMEM((1, width), f32),
            pltpu.VMEM((count, width), f32),
            pltpu.VMEM((ctxs, rows, pair), bf),
            pltpu.VMEM((pair, cached), bf),
            pltpu.VMEM((pair, cached), bf),
            pltpu.VMEM((cached, 2 * pair), bf),
            pltpu.VMEM((cached, 2 * pair), bf),
            pltpu.VMEM((2 * count, pair), bf),
            pltpu.VMEM((2 * count, 2 * pair), bf),
            pltpu.VMEM((rows, cached), f32),
            pltpu.VMEM((rows, cached), f32),
            pltpu.VMEM((2, rows, pair), f32),
            pltpu.VMEM((2, rows, pair), f32),
            pltpu.VMEM((rows, pair), f32),
            pltpu.VMEM((rows, pair), bf),
            pltpu.VMEM((rows, 2 * pair), f32),
            pltpu.VMEM((ctxs, rows, pair), bf),
            pltpu.VMEM((ctxs, 4, pair), f32),
            pltpu.VMEM((ctxs, rows, pair), bf),
            pltpu.VMEM((ctxs, 4, pair), f32),
            pltpu.VMEM(wo.shape, bf),
            pltpu.VMEM((heads - 1, count, width), bf),
            pltpu.VMEM((heads - 1, count, width), bf),
            pltpu.VMEM((3, hidden, model), bf),
            pltpu.VMEM((count, padded), f32),
            pltpu.VMEM((heads, 2 * padded, padded), bf),
            pltpu.VMEM((heads, padded, padded), bf),
            pltpu.VMEM((slots, count), bf),
            pltpu.VMEM((3, count, slots), bf),
            pltpu.VMEM((slots, padded), bf),
            pltpu.VMEM((heads, slots, padded), bf),
            pltpu.VMEM((slots, 2 * padded), f32),
            pltpu.VMEM((slots, padded), bf),
            pltpu.VMEM((heads - 1, GROUPS, block, padded), bf),
            pltpu.VMEM((heads - 1, GROUPS, block, padded), bf),
            pltpu.VMEM((slots, padded), bf),
            pltpu.VMEM((slots, padded), bf),
            dma((4 + spans,)),
            dma((5,)),
            dma((ctxs,)),
            dma((ctxs,)),
            dma((ctxs,)),
            dma((ctxs,)),
            dma((ctxs,)),
            dma((ctxs,)),
            dma((heads - 1,)),
            dma((heads - 1,)),
            dma((4,)),
            dma((experts,)),
            dma((experts,)),
            dma((heads, GROUPS)),
            dma((heads, GROUPS)),
            dma((heads - 1, GROUPS)),
            dma((heads - 1, GROUPS)),
            dma((experts,)),
            dma((experts,)),
        ],
        compiler_params=pltpu.CompilerParams(
            collective_id=0, has_side_effects=True, vmem_limit_bytes=56 * 1024 * 1024
        ),
    )(tokens, qw, kt, vt, nk, nv, wo, gain, ids, weights, gate, up, down)


def body(
    stream,
    query_weight,
    cache_keys,
    cache_values,
    new_keys,
    new_values,
    out_weight,
    norm_gain,
    expert_ids,
    expert_weights,
    gate_weight,
    up_weight,
    down_weight,
):
    heads = lax.axis_size("head")
    taken, model = out_weight.shape
    mixed = layer(
        stream[0],
        query_weight,
        cache_keys[0, :, 0, :].T,
        cache_values[0, :, 0, :].T,
        new_keys[0, :, 0, :],
        new_values[0, :, 0, :],
        out_weight.T.reshape(heads, model // heads, taken),
        norm_gain,
        expert_ids[0].T,
        expert_weights[0].T,
        gate_weight[0].T,
        up_weight[0].T,
        down_weight[0],
    )
    return mixed[None]


def solution(mesh):
    in_specs = (
        P("seq", "ctx", None),
        P(None, "head"),
        P("seq", "ctx", "head", None),
        P("seq", "ctx", "head", None),
        P("seq", "ctx", "head", None),
        P("seq", "ctx", "head", None),
        P("head", None),
        P(),
        P("seq", "ctx", None),
        P("seq", "ctx", None),
        P(("seq", "ctx"), None, "head"),
        P(("seq", "ctx"), None, "head"),
        P(("seq", "ctx"), "head", None),
    )
    out_specs = P("seq", "ctx", "head")
    return jax.shard_map(body, mesh=mesh, in_specs=in_specs, out_specs=out_specs, check_vma=False)
```
